16 devices in a mesh: dp: 2 (over y, z), cp: 8 (over x, core).
Axes of the slice: x: 4, y: 2, z: 1, core: 2. Of those that a mesh axis runs over, the one named last changes fastest.
The devices are a block of a 4x4x8 slice.
Arguments:
- x_in: bfloat16 [4096, 3072], P(('dp', 'cp')), parts along dimension 0
- dy_in: bfloat16 [4096, 3072], P(('dp', 'cp')), parts along dimension 0
- w_q: bfloat16 [3072, 3072], replicated
- w_k: bfloat16 [3072, 1024], replicated
- w_v: bfloat16 [3072, 1024], replicated
- w_o: bfloat16 [3072, 3072], replicated
Outputs:
- output 1: bfloat16 [4096, 3072], P(('dp', 'cp')), parts along dimension 0
- output 2: bfloat16 [4096, 3072], P(('dp', 'cp')), parts along dimension 0
There are 2 independent parts. The reference program is written for one: setup_inputs(seed, part) draws one part's arguments, and reference() takes and returns one part's arrays. A program takes and returns all parts, laid end to end along the dimension named above; an argument that names none is the same for every part.
All inputs are finite; a program needn't handle non-finite values.
Results may differ from the reference program's by a relative error of at most 0.0106845.
Values are sent between devices in bfloat16 or wider.
A program may use at most 768 MiB of HBM per device.

```python
import math
import jax
import jax.numpy as jnp
from jax import lax

SEQ_LEN = 2048
D_MODEL = 3072
Q_HEADS = 24
KV_HEADS = 8
HEAD_DIM = 128
QUERY_BLOCK = 128

Q_GROUP = Q_HEADS // KV_HEADS
SCORE_GAIN = (0.75 * math.log(SEQ_LEN)) ** 0.25


def setup_inputs(seed: int = 0, part: int = 0) -> dict:
    key_base = jax.random.key(seed)
    key_part = jax.random.fold_in(key_base, part)
    key_x, key_dy = jax.random.split(key_part)
    key_wq, key_wk, key_wv, key_wo = jax.random.split(jax.random.key(seed + 1), 4)
    in_scale = D_MODEL ** -0.5
    out_scale = (Q_HEADS * HEAD_DIM) ** -0.5
    x_in = jax.random.normal(key_x, (SEQ_LEN, D_MODEL), jnp.float32).astype(jnp.bfloat16)
    dy_in = jax.random.normal(key_dy, (SEQ_LEN, D_MODEL), jnp.float32).astype(jnp.bfloat16)
    w_q = (jax.random.normal(key_wq, (D_MODEL, Q_HEADS * HEAD_DIM), jnp.float32) * (in_scale * SCORE_GAIN)).astype(jnp.bfloat16)
    w_k = (jax.random.normal(key_wk, (D_MODEL, KV_HEADS * HEAD_DIM), jnp.float32) * (in_scale * SCORE_GAIN)).astype(jnp.bfloat16)
    w_v = (jax.random.normal(key_wv, (D_MODEL, KV_HEADS * HEAD_DIM), jnp.float32) * in_scale).astype(jnp.bfloat16)
    w_o = (jax.random.normal(key_wo, (Q_HEADS * HEAD_DIM, D_MODEL), jnp.float32) * out_scale).astype(jnp.bfloat16)
    return {"x_in": x_in, "dy_in": dy_in, "w_q": w_q, "w_k": w_k, "w_v": w_v, "w_o": w_o}


def project(rows_in, weight):
    return jnp.dot(rows_in, weight, preferred_element_type=jnp.float32).astype(jnp.bfloat16)


def reference(x_in, dy_in, w_q, w_k, w_v, w_o):
    score_scale = HEAD_DIM ** -0.5
    n_blocks = SEQ_LEN // QUERY_BLOCK
    q_rows = project(x_in, w_q).reshape(n_blocks, QUERY_BLOCK, KV_HEADS, Q_GROUP, HEAD_DIM)
    k_rows = project(x_in, w_k).reshape(SEQ_LEN, KV_HEADS, HEAD_DIM).astype(jnp.float32)
    v_rows = project(x_in, w_v).reshape(SEQ_LEN, KV_HEADS, HEAD_DIM).astype(jnp.float32)

    def forward_block(q_blk):
        q_f = q_blk.astype(jnp.float32)
        scores = jnp.einsum("thjd,uhd->thju", q_f, k_rows) * score_scale
        lse_blk = jax.nn.logsumexp(scores, axis=-1, keepdims=True)
        prob_bf = jnp.exp(scores - lse_blk).astype(jnp.bfloat16)
        out_blk = jnp.einsum("thju,uhd->thjd", prob_bf.astype(jnp.float32), v_rows).astype(jnp.bfloat16)
        return out_blk, lse_blk

    out_blocks, lse_blocks = lax.map(forward_block, q_rows)
    out_flat = out_blocks.reshape(SEQ_LEN, Q_HEADS * HEAD_DIM)
    y_out = project(out_flat, w_o)
    do_flat = jnp.dot(dy_in, w_o.T, preferred_element_type=jnp.float32).astype(jnp.bfloat16)
    do_blocks = do_flat.reshape(n_blocks, QUERY_BLOCK, KV_HEADS, Q_GROUP, HEAD_DIM)

    def backward_block(acc_pair, block_in):
        dk_acc, dv_acc = acc_pair
        q_blk, out_blk, do_blk, lse_blk = block_in
        q_f = q_blk.astype(jnp.float32)
        do_f = do_blk.astype(jnp.float32)
        scores = jnp.einsum("thjd,uhd->thju", q_f, k_rows) * score_scale
        prob_f = jnp.exp(scores - lse_blk).astype(jnp.bfloat16).astype(jnp.float32)
        row_delta = jnp.sum(do_f * out_blk.astype(jnp.float32), axis=-1, keepdims=True)
        dprob = jnp.einsum("thjd,uhd->thju", do_f, v_rows)
        dscore = (prob_f * (dprob - row_delta)).astype(jnp.bfloat16).astype(jnp.float32)
        dq_blk = (jnp.einsum("thju,uhd->thjd", dscore, k_rows) * score_scale).astype(jnp.bfloat16)
        dk_acc = dk_acc + jnp.einsum("thju,thjd->uhd", dscore, q_f) * score_scale
        dv_acc = dv_acc + jnp.einsum("thju,thjd->uhd", prob_f, do_f)
        return (dk_acc, dv_acc), dq_blk

    zero_acc = jnp.zeros((SEQ_LEN, KV_HEADS, HEAD_DIM), jnp.float32)
    acc_final, dq_blocks = lax.scan(backward_block, (zero_acc, zero_acc), (q_rows, out_blocks, do_blocks, lse_blocks))
    dq_flat = dq_blocks.reshape(SEQ_LEN, Q_HEADS * HEAD_DIM)
    dk_flat = acc_final[0].astype(jnp.bfloat16).reshape(SEQ_LEN, KV_HEADS * HEAD_DIM)
    dv_flat = acc_final[1].astype(jnp.bfloat16).reshape(SEQ_LEN, KV_HEADS * HEAD_DIM)
    dx_acc = (jnp.dot(dq_flat, w_q.T, preferred_element_type=jnp.float32)
              + jnp.dot(dk_flat, w_k.T, preferred_element_type=jnp.float32)
              + jnp.dot(dv_flat, w_v.T, preferred_element_type=jnp.float32))
    return y_out, dx_acc.astype(jnp.bfloat16)
```

```python
import functools

import jax
import jax.numpy as jnp
from jax import lax
from jax.experimental import pallas as pl
from jax.experimental.pallas import tpu as pltpu
from jax.sharding import PartitionSpec as P

HEAD_DIM = 128
CORES = 2
LOG2E = 1.4426950408889634
M_KV, M_Q, M_DO, M_O, M_DQ, M_DK, M_DV = range(7)
N_KINDS = 7
PARTS = 4
N_CHUNK = 4


def gray(q, n_chips):
    if n_chips != 4:
        return q
    return q + (q // 2) * (1 - 2 * (q % 2))


def dot_nn(a, b):
    return lax.dot_general(a, b, (((1,), (0,)), ((), ())), preferred_element_type=jnp.float32)


def dot_nt(a, b):
    return lax.dot_general(a, b, (((1,), (1,)), ((), ())), preferred_element_type=jnp.float32)


def body(n, rows, d_model, group,
         x_hbm, dy_hbm, wq_hbm, wk_hbm, wv_hbm, wo_hbm,
         y_hbm, dx_hbm,
         x_v, dy_v, wa, wb, kv_s, q_s, do_s, kv_r, q_r, do_r, kt, vt,
         o_s, dq_s, o_r, dq_r, dkt, dvt, dk_s, dv_s, dkv_r,
         s_v, p_v, dx_acc, out_v,
         in_sem, a_sem, b_sem, out_sem, send_sem, recv_sem):
    chips = n // CORES
    gw = group * HEAD_DIM
    cw = CORES * gw
    kw = CORES * HEAD_DIM
    tokens = n * rows
    kv_cols = n * HEAD_DIM
    scale = HEAD_DIM ** -0.5
    tiles = d_model // cw
    me = lax.axis_index("cp")
    chip = me // CORES
    core = me % CORES

    def peer_at(kind, src, dst, peer):
        return pltpu.make_async_remote_copy(
            src_ref=src, dst_ref=dst, send_sem=send_sem.at[kind, peer], recv_sem=recv_sem.at[kind, me],
            device_id={"cp": peer}, device_id_type=pl.DeviceIdType.MESH)

    def recv_wait(kind, dst, peer):
        pltpu.make_async_remote_copy(
            src_ref=dst, dst_ref=dst, send_sem=send_sem.at[kind, peer], recv_sem=recv_sem.at[kind, peer],
            device_id={"cp": peer}, device_id_type=pl.DeviceIdType.MESH).wait_recv()

    def rows_of(i):
        return pl.ds(pl.multiple_of(i * rows, rows), rows)

    def cols_of(i, w):
        return pl.ds(pl.multiple_of(i * w, w), w)

    def dest_chip(t):
        return (chip + gray((t + 1) % chips, chips)) % chips

    def start_parts(src, dst, sem, n_rows):
        step = n_rows // PARTS
        for i in range(PARTS):
            pltpu.make_async_copy(src.at[i * step:(i + 1) * step], dst.at[i * step:(i + 1) * step], sem).start()

    def load_kv(t):
        ch = dest_chip(t)
        a_t = wa.at[t % 2]
        start_parts(wk_hbm.at[:, cols_of(ch, kw)], a_t.at[:, 0:kw], a_sem.at[t % 2], d_model)
        start_parts(wv_hbm.at[:, cols_of(ch, kw)], a_t.at[:, kw:2 * kw], a_sem.at[t % 2], d_model)

    def load_q(t):
        start_parts(wq_hbm.at[:, cols_of(dest_chip(t), cw)], wa.at[t % 2], a_sem.at[t % 2], d_model)

    def load_y(t):
        start_parts(wo_hbm.at[:, cols_of(t, cw)], wa.at[t % 2], a_sem.at[t % 2], d_model)

    def load_do(t):
        start_parts(wo_hbm.at[cols_of(dest_chip(t), cw)], wb.at[t % 2], b_sem.at[t % 2], cw)

    def load_dxq(t):
        start_parts(wq_hbm.at[cols_of(t, cw)], wb.at[t % 2], b_sem.at[t % 2], cw)

    def load_dxkv(t):
        b_t = wb.at[t % 2]
        start_parts(wk_hbm.at[cols_of(t, cw)], b_t.at[:, 0:kv_cols], b_sem.at[t % 2], cw)
        start_parts(wv_hbm.at[cols_of(t, cw)], b_t.at[:, kv_cols:2 * kv_cols], b_sem.at[t % 2], cw)

    def wait_on(ref, sem):
        pltpu.make_async_copy(ref, ref, sem).wait()

    pltpu.make_async_copy(x_hbm, x_v, in_sem.at[0]).start()
    load_kv(0)
    load_kv(1)
    pltpu.make_async_copy(dy_hbm, dy_v, in_sem.at[1]).start()
    load_do(0)
    load_do(1)

    barrier = pltpu.get_barrier_semaphore()
    for r in range(1, n):
        pl.semaphore_signal(barrier, inc=1, device_id={"cp": (me + r) % n}, device_id_type=pl.DeviceIdType.MESH)
    pl.semaphore_wait(barrier, n - 1)

    wait_on(x_v, in_sem.at[0])

    def kv_step(t, carry):
        ch = dest_chip(t)
        wait_on(wa.at[t % 2, :, 0:2 * kw], a_sem.at[t % 2])
        res = dot_nn(x_v[...], wa[t % 2, :, 0:2 * kw]).astype(jnp.bfloat16)
        for c in range(CORES):
            kv_s[ch * CORES + c, :, 0:HEAD_DIM] = res[:, c * HEAD_DIM:(c + 1) * HEAD_DIM]
            kv_s[ch * CORES + c, :, HEAD_DIM:2 * HEAD_DIM] = res[:, kw + c * HEAD_DIM:kw + (c + 1) * HEAD_DIM]

        @pl.when(t + 2 < chips)
        def _():
            load_kv(t + 2)

        @pl.when(t + 2 >= chips)
        def _():
            load_q(t + 2 - chips)

        for c in range(CORES):
            peer = ch * CORES + (core + c) % CORES

            @pl.when(peer != me)
            def _():
                peer_at(M_KV, kv_s.at[peer], kv_r.at[rows_of(me)], peer).start()
        return carry

    lax.fori_loop(0, chips, kv_step, 0)
    wait_on(dy_v, in_sem.at[1])

    def send_heads(kind, stage, dest, ch):
        for c in range(CORES):
            peer = ch * CORES + (core + c) % CORES

            @pl.when(peer != me)
            def _():
                peer_at(kind, stage.at[peer], dest.at[rows_of(me)], peer).start()

    def qdo_step(t, carry):
        ch = dest_chip(t)
        wait_on(wa.at[t % 2], a_sem.at[t % 2])
        res = dot_nn(x_v[...], wa[t % 2]).astype(jnp.bfloat16)
        for c in range(CORES):
            q_s[ch * CORES + c] = res[:, c * gw:(c + 1) * gw]

        @pl.when(t + 2 < chips)
        def _():
            load_q(t + 2)

        @pl.when(t + 2 >= chips)
        def _():
            load_y(t + 2 - chips)

        send_heads(M_Q, q_s, q_r, ch)
        wait_on(wb.at[t % 2], b_sem.at[t % 2])
        res2 = dot_nt(dy_v[...], wb[t % 2]).astype(jnp.bfloat16)
        for c in range(CORES):
            do_s[ch * CORES + c] = res2[:, c * gw:(c + 1) * gw]

        @pl.when(t + 2 < chips)
        def _():
            load_do(t + 2)

        @pl.when(t + 2 >= chips)
        def _():
            load_dxq(t + 2 - chips)

        send_heads(M_DO, do_s, do_r, ch)
        return carry

    lax.fori_loop(0, chips, qdo_step, 0)

    kv_r[rows_of(me), :] = kv_s[me]
    q_r[rows_of(me), :] = q_s[me]
    do_r[rows_of(me), :] = do_s[me]
    dkt[...] = jnp.zeros_like(dkt)
    dvt[...] = jnp.zeros_like(dvt)

    for r in range(1, n):
        src = (me + r) % n
        recv_wait(M_KV, kv_r.at[rows_of(src)], src)

    def turn(j, carry):
        kt[:, cols_of(j, rows)] = kv_r[rows_of(j), 0:HEAD_DIM].T
        vt[:, cols_of(j, rows)] = kv_r[rows_of(j), HEAD_DIM:2 * HEAD_DIM].T
        return carry

    lax.fori_loop(0, n, turn, 0)

    width = tokens // N_CHUNK
    kk = scale * LOG2E

    def attend(it, carry):
        k = it // group
        g = it % group
        src = ((chip - gray(k // CORES, chips) + chips) % chips) * CORES + (core + k % CORES) % CORES

        @pl.when((g == 0) & (k > 0))
        def _():
            recv_wait(M_Q, q_r.at[rows_of(src)], src)
            recv_wait(M_DO, do_r.at[rows_of(src)], src)

        head = cols_of(g, HEAD_DIM)
        q_blk = q_r[rows_of(src), head]
        do_blk = do_r[rows_of(src), head]
        top = None
        for i in range(N_CHUNK):
            s_i = dot_nn(q_blk, kt[:, i * width:(i + 1) * width])
            s_v[:, i * width:(i + 1) * width] = s_i
            for j in range(width // 128):
                part = s_i[:, j * 128:(j + 1) * 128]
                top = part if top is None else jnp.maximum(top, part)
        top = jnp.max(top, axis=1, keepdims=True) * kk
        total = None
        for i in range(N_CHUNK):
            e_i = jnp.exp2(s_v[:, i * width:(i + 1) * width] * kk - top)
            s_v[:, i * width:(i + 1) * width] = e_i
            for j in range(width // 128):
                part = e_i[:, j * 128:(j + 1) * 128]
                total = part if total is None else total + part
        inv = 1.0 / jnp.sum(total, axis=1, keepdims=True)
        out = None
        for i in range(N_CHUNK):
            p_i = (s_v[:, i * width:(i + 1) * width] * inv).astype(jnp.bfloat16)
            p_v[:, i * width:(i + 1) * width] = p_i
            part = dot_nn(p_i, kv_r[i * width:(i + 1) * width, HEAD_DIM:2 * HEAD_DIM])
            out = part if out is None else out + part
        out_b = out.astype(jnp.bfloat16)
        o_s[rows_of(src), head] = out_b
        delta = jnp.sum(do_blk.astype(jnp.float32) * out_b.astype(jnp.float32), axis=1, keepdims=True)
        q_t = q_blk.T
        do_t = do_blk.T
        dq = None
        for i in range(N_CHUNK):
            sl = slice(i * width, (i + 1) * width)
            dp = dot_nn(do_blk, vt[:, sl])
            p_i = p_v[:, sl]
            ds = (p_i.astype(jnp.float32) * (dp - delta)).astype(jnp.bfloat16)
            part = dot_nn(ds, kv_r[sl, 0:HEAD_DIM])
            dq = part if dq is None else dq + part
            dkt[:, sl] += dot_nn(q_t, ds)
            dvt[:, sl] += dot_nn(do_t, p_i)
        dq_s[rows_of(src), head] = (dq * scale).astype(jnp.bfloat16)

        @pl.when((g == group - 1) & (k > 0))
        def _():
            peer_at(M_O, o_s.at[rows_of(src)], o_r.at[:, cols_of(me, gw)], src).start()
            peer_at(M_DQ, dq_s.at[rows_of(src)], dq_r.at[:, cols_of(me, gw)], src).start()
        return carry

    lax.fori_loop(0, n * group, attend, 0)

    def finish(j, carry):
        off = n - 1 - j
        dst = ((chip + off // CORES) % chips) * CORES + (core + off % CORES) % CORES
        dk_s[dst] = (dkt[:, cols_of(dst, rows)] * scale).T.astype(jnp.bfloat16)
        dv_s[dst] = dvt[:, cols_of(dst, rows)].T.astype(jnp.bfloat16)

        @pl.when(dst != me)
        def _():
            peer_at(M_DK, dk_s.at[dst], dkv_r.at[:, cols_of(me, HEAD_DIM)], dst).start()
            peer_at(M_DV, dv_s.at[dst], dkv_r.at[:, pl.ds(pl.multiple_of(kv_cols + me * HEAD_DIM, HEAD_DIM), HEAD_DIM)], dst).start()
        return carry

    lax.fori_loop(0, n, finish, 0)

    o_r[:, cols_of(me, gw)] = o_s[rows_of(me), :]
    dq_r[:, cols_of(me, gw)] = dq_s[rows_of(me), :]
    dkv_r[:, cols_of(me, HEAD_DIM)] = dk_s[me]
    dkv_r[:, pl.ds(pl.multiple_of(kv_cols + me * HEAD_DIM, HEAD_DIM), HEAD_DIM)] = dv_s[me]
    for r in range(1, n):
        src = (me + r) % n
        recv_wait(M_O, o_r.at[:, cols_of(src, gw)], src)

    def put_out(t, hbm, value):
        @pl.when(t >= 2)
        def _():
            wait_on(out_v.at[t % 2], out_sem.at[t % 2])

        out_v[t % 2] = value
        pltpu.make_async_copy(out_v.at[t % 2], hbm.at[:, cols_of(t, cw)], out_sem.at[t % 2]).start()

    def drain_out():
        for i in range(2):
            wait_on(out_v.at[i], out_sem.at[i])

    def y_step(t, carry):
        wait_on(wa.at[t % 2], a_sem.at[t % 2])
        res = dot_nn(o_r[...], wa[t % 2]).astype(jnp.bfloat16)

        @pl.when(t + 2 < tiles)
        def _():
            load_y(t + 2)

        put_out(t, y_hbm, res)
        return carry

    lax.fori_loop(0, tiles, y_step, 0)
    drain_out()

    for r in range(1, n):
        src = (me + r) % n
        recv_wait(M_DQ, dq_r.at[:, cols_of(src, gw)], src)

    def dxq_step(t, carry):
        wait_on(wb.at[t % 2], b_sem.at[t % 2])
        dx_acc[:, cols_of(t, cw)] = dot_nt(dq_r[...], wb[t % 2])

        @pl.when(t + 2 < tiles)
        def _():
            load_dxq(t + 2)

        @pl.when(t + 2 >= tiles)
        def _():
            load_dxkv(t + 2 - tiles)
        return carry

    lax.fori_loop(0, tiles, dxq_step, 0)

    for r in range(1, n):
        src = (me + r) % n
        recv_wait(M_DK, dkv_r.at[:, cols_of(src, HEAD_DIM)], src)
        recv_wait(M_DV, dkv_r.at[:, pl.ds(pl.multiple_of(kv_cols + src * HEAD_DIM, HEAD_DIM), HEAD_DIM)], src)

    def dxkv_step(t, carry):
        wait_on(wb.at[t % 2, :, 0:2 * kv_cols], b_sem.at[t % 2])
        res = (dx_acc[:, cols_of(t, cw)] + dot_nt(dkv_r[...], wb[t % 2, :, 0:2 * kv_cols])).astype(jnp.bfloat16)

        @pl.when(t + 2 < tiles)
        def _():
            load_dxkv(t + 2)

        put_out(t, dx_hbm, res)
        return carry

    lax.fori_loop(0, tiles, dxkv_step, 0)
    drain_out()

    for r in range(1, n):
        peer = (me + r) % n
        peer_at(M_KV, kv_s.at[peer], kv_r.at[rows_of(me)], peer).wait_send()
        peer_at(M_Q, q_s.at[peer], q_r.at[rows_of(me)], peer).wait_send()
        peer_at(M_DO, do_s.at[peer], do_r.at[rows_of(me)], peer).wait_send()
        peer_at(M_O, o_s.at[rows_of(peer)], o_r.at[:, cols_of(me, gw)], peer).wait_send()
        peer_at(M_DQ, dq_s.at[rows_of(peer)], dq_r.at[:, cols_of(me, gw)], peer).wait_send()
        peer_at(M_DK, dk_s.at[peer], dkv_r.at[:, cols_of(me, HEAD_DIM)], peer).wait_send()
        peer_at(M_DV, dv_s.at[peer], dkv_r.at[:, pl.ds(pl.multiple_of(kv_cols + me * HEAD_DIM, HEAD_DIM), HEAD_DIM)], peer).wait_send()


def solution(mesh):
    n = mesh.shape["cp"]
    row_spec = P(("dp", "cp"), None)
    full_spec = P(None, None)

    def local_body(x_loc, dy_loc, w_q, w_k, w_v, w_o):
        rows, d_model = x_loc.shape
        q_heads = w_q.shape[1] // HEAD_DIM
        kv_heads = w_k.shape[1] // HEAD_DIM
        group = q_heads // kv_heads
        assert kv_heads == n and n % CORES == 0
        gw = group * HEAD_DIM
        cw = CORES * gw
        tokens = n * rows
        bf, f32 = jnp.bfloat16, jnp.float32
        vm = pltpu.VMEM
        scratch = [
            vm((rows, d_model), bf), vm((rows, d_model), bf),
            vm((2, d_model, cw), bf), vm((2, cw, d_model), bf),
            vm((n, rows, 2 * HEAD_DIM), bf), vm((n, rows, gw), bf), vm((n, rows, gw), bf),
            vm((tokens, 2 * HEAD_DIM), bf), vm((tokens, gw), bf), vm((tokens, gw), bf),
            vm((HEAD_DIM, tokens), bf), vm((HEAD_DIM, tokens), bf),
            vm((tokens, gw), bf), vm((tokens, gw), bf),
            vm((rows, n * gw), bf), vm((rows, n * gw), bf),
            vm((HEAD_DIM, tokens), f32), vm((HEAD_DIM, tokens), f32),
            vm((n, rows, HEAD_DIM), bf), vm((n, rows, HEAD_DIM), bf),
            vm((rows, 2 * n * HEAD_DIM), bf),
            vm((rows, tokens), f32), vm((rows, tokens), bf),
            vm((rows, d_model), f32), vm((2, rows, cw), bf),
            pltpu.SemaphoreType.DMA((2,)), pltpu.SemaphoreType.DMA((2,)), pltpu.SemaphoreType.DMA((2,)),
            pltpu.SemaphoreType.DMA((2,)),
            pltpu.SemaphoreType.DMA((N_KINDS, n)), pltpu.SemaphoreType.DMA((N_KINDS, n)),
        ]
        out = jax.ShapeDtypeStruct((rows, d_model), bf)
        return pl.pallas_call(
            functools.partial(body, n, rows, d_model, group),
            out_shape=(out, out),
            in_specs=[pl.BlockSpec(memory_space=pl.ANY)] * 6,
            out_specs=(pl.BlockSpec(memory_space=pl.ANY), pl.BlockSpec(memory_space=pl.ANY)),
            scratch_shapes=scratch,
            compiler_params=pltpu.CompilerParams(collective_id=0, has_side_effects=True,
                                                 vmem_limit_bytes=63 * 1024 * 1024),
        )(x_loc, dy_loc, w_q, w_k, w_v, w_o)

    return jax.shard_map(local_body, mesh=mesh,
                         in_specs=(row_spec, row_spec, full_spec, full_spec, full_spec, full_spec),
                         out_specs=(row_spec, row_spec), check_vma=False)
```

```python
import functools

import jax
import jax.numpy as jnp
from jax import lax
from jax.experimental import pallas as pl
from jax.experimental.pallas import tpu as pltpu
from jax.sharding import PartitionSpec as P

HEAD_DIM = 128
CORES = 2
LOG2E = 1.4426950408889634
M_KV, M_Q, M_DO, M_O, M_DQ, M_DK, M_DV = range(7)
N_KINDS = 7
PARTS = 4
CHUNK = 1024


def gray(q, n_chips):
    if n_chips != 4:
        return q
    return q + (q // 2) * (1 - 2 * (q % 2))


def dot_nn(a, b):
    return lax.dot_general(a, b, (((1,), (0,)), ((), ())), preferred_element_type=jnp.float32)


def dot_nt(a, b):
    return lax.dot_general(a, b, (((1,), (1,)), ((), ())), preferred_element_type=jnp.float32)


def body(n, rows, d_model, group,
         x_hbm, dy_hbm, wq_hbm, wk_hbm, wv_hbm, wo_hbm,
         y_hbm, dx_hbm,
         x_v, dy_v, wa, wb, kv_s, q_s, do_s, kv_r, q_r, do_r, kt, vt,
         o_s, dq_s, o_r, dq_r, dk_v, dv_v, dk_s, dv_s, dkv_r,
         s_v, p_v, ds_v, out_v,
         in_sem, a_sem, b_sem, out_sem, send_sem, recv_sem):
    chips = n // CORES
    gw = group * HEAD_DIM
    cw = CORES * gw
    kw = CORES * HEAD_DIM
    tokens = n * rows
    kv_cols = n * HEAD_DIM
    scale = HEAD_DIM ** -0.5
    tiles = d_model // cw
    me = lax.axis_index("cp")
    chip = me // CORES
    core = me % CORES

    def peer_at(kind, src, dst, peer):
        return pltpu.make_async_remote_copy(
            src_ref=src, dst_ref=dst, send_sem=send_sem.at[kind, peer], recv_sem=recv_sem.at[kind, me],
            device_id={"cp": peer}, device_id_type=pl.DeviceIdType.MESH)

    def recv_wait(kind, dst, peer):
        pltpu.make_async_remote_copy(
            src_ref=dst, dst_ref=dst, send_sem=send_sem.at[kind, peer], recv_sem=recv_sem.at[kind, peer],
            device_id={"cp": peer}, device_id_type=pl.DeviceIdType.MESH).wait_recv()

    def rows_of(i):
        return pl.ds(pl.multiple_of(i * rows, rows), rows)

    def cols_of(i, w):
        return pl.ds(pl.multiple_of(i * w, w), w)

    def dest_chip(t):
        return (chip + gray((t + 1) % chips, chips)) % chips

    def start_parts(src, dst, sem, n_rows):
        step = n_rows // PARTS
        for i in range(PARTS):
            pltpu.make_async_copy(src.at[i * step:(i + 1) * step], dst.at[i * step:(i + 1) * step], sem).start()

    def load_kv(t):
        ch = dest_chip(t)
        a_t = wa.at[t % 2]
        start_parts(wk_hbm.at[:, cols_of(ch, kw)], a_t.at[:, 0:kw], a_sem.at[t % 2], d_model)
        start_parts(wv_hbm.at[:, cols_of(ch, kw)], a_t.at[:, kw:2 * kw], a_sem.at[t % 2], d_model)

    def load_q(t):
        start_parts(wq_hbm.at[:, cols_of(dest_chip(t), cw)], wa.at[t % 2], a_sem.at[t % 2], d_model)

    def load_y(t):
        start_parts(wo_hbm.at[:, cols_of(t, cw)], wa.at[t % 2], a_sem.at[t % 2], d_model)

    def load_do(t):
        start_parts(wo_hbm.at[cols_of(dest_chip(t), cw)], wb.at[t % 2], b_sem.at[t % 2], cw)

    def load_dxq(t):
        start_parts(wq_hbm.at[cols_of(t, cw)], wb.at[t % 2], b_sem.at[t % 2], cw)

    def load_dxkv(t):
        b_t = wb.at[t % 2]
        start_parts(wk_hbm.at[cols_of(t, cw)], b_t.at[:, 0:kv_cols], b_sem.at[t % 2], cw)
        start_parts(wv_hbm.at[cols_of(t, cw)], b_t.at[:, kv_cols:2 * kv_cols], b_sem.at[t % 2], cw)

    def wait_on(ref, sem):
        pltpu.make_async_copy(ref, ref, sem).wait()

    pltpu.make_async_copy(x_hbm, x_v, in_sem.at[0]).start()
    load_kv(0)
    load_kv(1)
    pltpu.make_async_copy(dy_hbm, dy_v, in_sem.at[1]).start()
    load_do(0)
    load_do(1)

    barrier = pltpu.get_barrier_semaphore()
    for r in range(1, n):
        pl.semaphore_signal(barrier, inc=1, device_id={"cp": (me + r) % n}, device_id_type=pl.DeviceIdType.MESH)
    pl.semaphore_wait(barrier, n - 1)

    wait_on(x_v, in_sem.at[0])

    def kv_step(t, carry):
        ch = dest_chip(t)
        wait_on(wa.at[t % 2, :, 0:2 * kw], a_sem.at[t % 2])
        res = dot_nn(x_v[...], wa[t % 2, :, 0:2 * kw]).astype(jnp.bfloat16)
        for c in range(CORES):
            kv_s[ch * CORES + c, :, 0:HEAD_DIM] = res[:, c * HEAD_DIM:(c + 1) * HEAD_DIM]
            kv_s[ch * CORES + c, :, HEAD_DIM:2 * HEAD_DIM] = res[:, kw + c * HEAD_DIM:kw + (c + 1) * HEAD_DIM]

        @pl.when(t + 2 < chips)
        def _():
            load_kv(t + 2)

        @pl.when(t + 2 >= chips)
        def _():
            load_q(t + 2 - chips)

        for c in range(CORES):
            peer = ch * CORES + (core + c) % CORES

            @pl.when(peer != me)
            def _():
                peer_at(M_KV, kv_s.at[peer], kv_r.at[rows_of(me)], peer).start()
        return carry

    lax.fori_loop(0, chips, kv_step, 0)
    wait_on(dy_v, in_sem.at[1])

    def send_heads(kind, stage, dest, ch):
        for c in range(CORES):
            peer = ch * CORES + (core + c) % CORES

            @pl.when(peer != me)
            def _():
                peer_at(kind, stage.at[peer], dest.at[rows_of(me)], peer).start()

    def qdo_step(t, carry):
        ch = dest_chip(t)
        wait_on(wa.at[t % 2], a_sem.at[t % 2])
        res = dot_nn(x_v[...], wa[t % 2]).astype(jnp.bfloat16)
        for c in range(CORES):
            q_s[ch * CORES + c] = res[:, c * gw:(c + 1) * gw]

        @pl.when(t + 2 < chips)
        def _():
            load_q(t + 2)

        @pl.when(t + 2 >= chips)
        def _():
            load_y(t + 2 - chips)

        send_heads(M_Q, q_s, q_r, ch)
        wait_on(wb.at[t % 2], b_sem.at[t % 2])
        res2 = dot_nt(dy_v[...], wb[t % 2]).astype(jnp.bfloat16)
        for c in range(CORES):
            do_s[ch * CORES + c] = res2[:, c * gw:(c + 1) * gw]

        @pl.when(t + 2 < chips)
        def _():
            load_do(t + 2)

        @pl.when(t + 2 >= chips)
        def _():
            load_dxq(t + 2 - chips)

        send_heads(M_DO, do_s, do_r, ch)
        return carry

    lax.fori_loop(0, chips, qdo_step, 0)

    kv_r[rows_of(me), :] = kv_s[me]
    q_r[rows_of(me), :] = q_s[me]
    do_r[rows_of(me), :] = do_s[me]
    dk_v[...] = jnp.zeros_like(dk_v)
    dv_v[...] = jnp.zeros_like(dv_v)

    for r in range(1, n):
        src = (me + r) % n
        recv_wait(M_KV, kv_r.at[rows_of(src)], src)

    def turn(j, carry):
        kt[:, cols_of(j, rows)] = kv_r[rows_of(j), 0:HEAD_DIM].T
        vt[:, cols_of(j, rows)] = kv_r[rows_of(j), HEAD_DIM:2 * HEAD_DIM].T
        return carry

    lax.fori_loop(0, n, turn, 0)

    kk = scale * LOG2E
    chunks = [slice(i * CHUNK, (i + 1) * CHUNK) for i in range(tokens // CHUNK)]
    k_cols, v_cols = slice(0, HEAD_DIM), slice(HEAD_DIM, 2 * HEAD_DIM)

    def source(k):
        return ((chip - gray(k // CORES, chips) + chips) % chips) * CORES + (core + k % CORES) % CORES

    def by_eights(value):
        return value.reshape(value.shape[0] // 8, 8, value.shape[1])

    def score_steps(k, probs):
        src = source(k)
        for g in range(group):
            s_ref = s_v.at[g % 2]
            st = {}

            def first(g=g, st=st):
                st["q_t"] = q_r[rows_of(src), g * HEAD_DIM:(g + 1) * HEAD_DIM].T
                st["top"] = None

            def product(sl, s_ref=s_ref, st=st):
                s_i = dot_nn(kv_r[sl, k_cols], st["q_t"])
                s_ref[sl, :] = s_i
                top = jnp.max(by_eights(s_i), axis=0)
                st["top"] = top if st["top"] is None else jnp.maximum(st["top"], top)

            def shift(st=st):
                st["mk"] = jnp.max(st["top"], axis=0, keepdims=True) * kk
                st["sum"] = None

            def add(sl, s_ref=s_ref, st=st):
                part = jnp.sum(by_eights(jnp.exp2(s_ref[sl, :] * kk - st["mk"])), axis=0)
                st["sum"] = part if st["sum"] is None else st["sum"] + part

            def close(st=st):
                st["lse"] = st["mk"] + jnp.log2(jnp.sum(st["sum"], axis=0, keepdims=True))

            def emit(sl, g=g, s_ref=s_ref, st=st):
                probs[g, sl, :] = jnp.exp2(s_ref[sl, :] * kk - st["lse"]).astype(jnp.bfloat16)

            yield 1, first
            for sl in chunks:
                yield 6, functools.partial(product, sl)
            yield 1, shift
            for sl in chunks:
                yield 6, functools.partial(add, sl)
            yield 1, close
            for sl in chunks:
                yield 6, functools.partial(emit, sl)

    def grad_steps(k, probs):
        src = source(k)
        for g in range(group):
            st = {}
            head = slice(g * HEAD_DIM, (g + 1) * HEAD_DIM)

            def outputs(g=g, head=head, st=st):
                do_t = do_r[rows_of(src), head].T
                o_t = dot_nn(vt[...], probs[g]).astype(jnp.bfloat16)
                o_s[rows_of(src), head] = o_t.T
                st["do_t"] = do_t
                st["delta"] = jnp.sum(do_t.astype(jnp.float32) * o_t.astype(jnp.float32), axis=0, keepdims=True)

            def dscore(sl, g=g, st=st):
                dp = dot_nn(kv_r[sl, v_cols], st["do_t"])
                ds_v[g, sl, :] = (probs[g, sl, :].astype(jnp.float32) * (dp - st["delta"])).astype(jnp.bfloat16)

            def dquery(g=g, head=head):
                dq_t = (dot_nn(kt[...], ds_v[g]) * scale).astype(jnp.bfloat16)
                dq_s[rows_of(src), head] = dq_t.T

            yield 12, outputs
            for sl in chunks:
                yield 4, functools.partial(dscore, sl)
            yield 10, dquery

        def accumulate(acc, left, right_ref, sl):
            total = acc[sl, :]
            part = None
            for g in range(group):
                term = dot_nn(left[g, sl, :], right_ref[rows_of(src), g * HEAD_DIM:(g + 1) * HEAD_DIM])
                part = term if part is None else part + term
            acc[sl, :] = total + part

        for sl in chunks:
            yield 12, functools.partial(accumulate, dv_v, probs, do_r, sl)
        for sl in chunks:
            yield 12, functools.partial(accumulate, dk_v, ds_v, q_r, sl)

    def run_steps(*streams):
        lists = [list(s) for s in streams]
        totals = [sum(w for w, _ in s) for s in lists]
        tagged = []
        for order, (steps, whole) in enumerate(zip(lists, totals)):
            at = 0
            for w, f in steps:
                tagged.append(((at + w / 2) / whole, order, len(tagged), f))
                at += w
        for _, _, _, f in sorted(tagged, key=lambda t: t[:3]):
            f()

    def need(kind, dest, k):
        src = source(k)

        @pl.when((k > 0) & (k < n))
        def _():
            recv_wait(kind, dest.at[rows_of(src)], src)


    def attend(k, carry):
        need(M_Q, q_r, k)
        need(M_DO, do_r, k)
        run_steps(score_steps(k, p_v.at[0])); run_steps(grad_steps(k, p_v.at[0]))
        src = source(k)

        @pl.when(k > 0)
        def _():
            peer_at(M_O, o_s.at[rows_of(src)], o_r.at[:, cols_of(me, gw)], src).start()
            peer_at(M_DQ, dq_s.at[rows_of(src)], dq_r.at[:, cols_of(me, gw)], src).start()
        return carry

    lax.fori_loop(0, n, attend, 0)

    def finish(j, carry):
        off = n - 1 - j
        dst = ((chip + off // CORES) % chips) * CORES + (core + off % CORES) % CORES
        dk_s[dst] = (dk_v[rows_of(dst), :] * scale).astype(jnp.bfloat16)
        dv_s[dst] = dv_v[rows_of(dst), :].astype(jnp.bfloat16)

        @pl.when(dst != me)
        def _():
            peer_at(M_DK, dk_s.at[dst], dkv_r.at[:, cols_of(me, HEAD_DIM)], dst).start()
            peer_at(M_DV, dv_s.at[dst], dkv_r.at[:, pl.ds(pl.multiple_of(kv_cols + me * HEAD_DIM, HEAD_DIM), HEAD_DIM)], dst).start()
        return carry

    lax.fori_loop(0, n, finish, 0)

    o_r[:, cols_of(me, gw)] = o_s[rows_of(me), :]
    dq_r[:, cols_of(me, gw)] = dq_s[rows_of(me), :]
    dkv_r[:, cols_of(me, HEAD_DIM)] = dk_s[me]
    dkv_r[:, pl.ds(pl.multiple_of(kv_cols + me * HEAD_DIM, HEAD_DIM), HEAD_DIM)] = dv_s[me]
    for r in range(1, n):
        src = (me + r) % n
        recv_wait(M_O, o_r.at[:, cols_of(src, gw)], src)

    def put_out(t, hbm, value):
        @pl.when(t >= 2)
        def _():
            wait_on(out_v.at[t % 2], out_sem.at[t % 2])

        out_v[t % 2] = value
        pltpu.make_async_copy(out_v.at[t % 2], hbm.at[:, cols_of(t, cw)], out_sem.at[t % 2]).start()

    def drain_out():
        for i in range(2):
            wait_on(out_v.at[i], out_sem.at[i])

    def y_step(t, carry):
        wait_on(wa.at[t % 2], a_sem.at[t % 2])
        res = dot_nn(o_r[...], wa[t % 2]).astype(jnp.bfloat16)

        @pl.when(t + 2 < tiles)
        def _():
            load_y(t + 2)

        put_out(t, y_hbm, res)
        return carry

    lax.fori_loop(0, tiles, y_step, 0)
    drain_out()

    for r in range(1, n):
        src = (me + r) % n
        recv_wait(M_DQ, dq_r.at[:, cols_of(src, gw)], src)

    def dx_place(t, c):
        piece = t * (cw // rows) + c
        return piece // n, rows_of(piece % n)

    def dxq_step(t, carry):
        wait_on(wb.at[t % 2], b_sem.at[t % 2])
        res = dot_nt(dq_r[...], wb[t % 2])
        for c in range(cw // rows):
            s_v[dx_place(t, c)] = res[:, c * rows:(c + 1) * rows]

        @pl.when(t + 2 < tiles)
        def _():
            load_dxq(t + 2)

        @pl.when(t + 2 >= tiles)
        def _():
            load_dxkv(t + 2 - tiles)
        return carry

    lax.fori_loop(0, tiles, dxq_step, 0)

    for r in range(1, n):
        src = (me + r) % n
        recv_wait(M_DK, dkv_r.at[:, cols_of(src, HEAD_DIM)], src)
        recv_wait(M_DV, dkv_r.at[:, pl.ds(pl.multiple_of(kv_cols + src * HEAD_DIM, HEAD_DIM), HEAD_DIM)], src)

    def dxkv_step(t, carry):
        wait_on(wb.at[t % 2, :, 0:2 * kv_cols], b_sem.at[t % 2])
        res = dot_nt(dkv_r[...], wb[t % 2, :, 0:2 * kv_cols])
        res = jnp.concatenate([s_v[dx_place(t, c)] + res[:, c * rows:(c + 1) * rows] for c in range(cw // rows)], axis=1)
        res = res.astype(jnp.bfloat16)

        @pl.when(t + 2 < tiles)
        def _():
            load_dxkv(t + 2)

        put_out(t, dx_hbm, res)
        return carry

    lax.fori_loop(0, tiles, dxkv_step, 0)
    drain_out()

    for r in range(1, n):
        peer = (me + r) % n
        peer_at(M_KV, kv_s.at[peer], kv_r.at[rows_of(me)], peer).wait_send()
        peer_at(M_Q, q_s.at[peer], q_r.at[rows_of(me)], peer).wait_send()
        peer_at(M_DO, do_s.at[peer], do_r.at[rows_of(me)], peer).wait_send()
        peer_at(M_O, o_s.at[rows_of(peer)], o_r.at[:, cols_of(me, gw)], peer).wait_send()
        peer_at(M_DQ, dq_s.at[rows_of(peer)], dq_r.at[:, cols_of(me, gw)], peer).wait_send()
        peer_at(M_DK, dk_s.at[peer], dkv_r.at[:, cols_of(me, HEAD_DIM)], peer).wait_send()
        peer_at(M_DV, dv_s.at[peer], dkv_r.at[:, pl.ds(pl.multiple_of(kv_cols + me * HEAD_DIM, HEAD_DIM), HEAD_DIM)], peer).wait_send()


def solution(mesh):
    n = mesh.shape["cp"]
    row_spec = P(("dp", "cp"), None)
    full_spec = P(None, None)

    def local_body(x_loc, dy_loc, w_q, w_k, w_v, w_o):
        rows, d_model = x_loc.shape
        q_heads = w_q.shape[1] // HEAD_DIM
        kv_heads = w_k.shape[1] // HEAD_DIM
        group = q_heads // kv_heads
        assert kv_heads == n and n % CORES == 0
        gw = group * HEAD_DIM
        cw = CORES * gw
        tokens = n * rows
        bf, f32 = jnp.bfloat16, jnp.float32
        vm = pltpu.VMEM
        scratch = [
            vm((rows, d_model), bf), vm((rows, d_model), bf),
            vm((2, d_model, cw), bf), vm((2, cw, d_model), bf),
            vm((n, rows, 2 * HEAD_DIM), bf), vm((n, rows, gw), bf), vm((n, rows, gw), bf),
            vm((tokens, 2 * HEAD_DIM), bf), vm((tokens, gw), bf), vm((tokens, gw), bf),
            vm((HEAD_DIM, tokens), bf), vm((HEAD_DIM, tokens), bf),
            vm((tokens, gw), bf), vm((tokens, gw), bf),
            vm((rows, n * gw), bf), vm((rows, n * gw), bf),
            vm((tokens, HEAD_DIM), f32), vm((tokens, HEAD_DIM), f32),
            vm((n, rows, HEAD_DIM), bf), vm((n, rows, HEAD_DIM), bf),
            vm((rows, 2 * n * HEAD_DIM), bf),
            vm((2, tokens, rows), f32),
            vm((2, group, tokens, rows), bf), vm((group, tokens, rows), bf),
            vm((2, rows, cw), bf),
            pltpu.SemaphoreType.DMA((2,)), pltpu.SemaphoreType.DMA((2,)), pltpu.SemaphoreType.DMA((2,)),
            pltpu.SemaphoreType.DMA((2,)),
            pltpu.SemaphoreType.DMA((N_KINDS, n)), pltpu.SemaphoreType.DMA((N_KINDS, n)),
        ]
        out = jax.ShapeDtypeStruct((rows, d_model), bf)
        return pl.pallas_call(
            functools.partial(body, n, rows, d_model, group),
            out_shape=(out, out),
            in_specs=[pl.BlockSpec(memory_space=pl.ANY)] * 6,
            out_specs=(pl.BlockSpec(memory_space=pl.ANY), pl.BlockSpec(memory_space=pl.ANY)),
            scratch_shapes=scratch,
            compiler_params=pltpu.CompilerParams(collective_id=0, has_side_effects=True,
                                                 vmem_limit_bytes=63 * 1024 * 1024),
        )(x_loc, dy_loc, w_q, w_k, w_v, w_o)

    return jax.shard_map(local_body, mesh=mesh,
                         in_specs=(row_spec, row_spec, full_spec, full_spec, full_spec, full_spec),
                         out_specs=(row_spec, row_spec), check_vma=False)
```

```python
import functools

import jax
import jax.numpy as jnp
from jax import lax
from jax.experimental import pallas as pl
from jax.experimental.pallas import tpu as pltpu
from jax.sharding import PartitionSpec as P

HEAD_DIM = 128
CORES = 2
LOG2E = 1.4426950408889634
M_KV, M_Q, M_DO, M_O, M_DQ, M_DK, M_DV = range(7)
N_KINDS = 7
PARTS = 4
PIECE = 3
CHUNK = 1024


def gray(q, n_chips):
    if n_chips != 4:
        return q
    return q + (q // 2) * (1 - 2 * (q % 2))


def dot_nn(a, b):
    return lax.dot_general(a, b, (((1,), (0,)), ((), ())), preferred_element_type=jnp.float32)


def dot_nt(a, b):
    return lax.dot_general(a, b, (((1,), (1,)), ((), ())), preferred_element_type=jnp.float32)


def body(n, rows, d_model, group,
         x_hbm, dy_hbm, wq_hbm, wk_hbm, wv_hbm, wo_hbm,
         y_hbm, dx_hbm,
         x_v, dy_v, wa, wb, kv_s, q_s, do_s, kv_r, q_r, do_r, kt, vt,
         o_s, dq_s, o_r, dq_r, dk_v, dv_v, dk_s, dv_s, dkv_r,
         s_v, p_v, ds_v, y_acc, out_v,
         in_sem, a_sem, b_sem, out_sem, send_sem, recv_sem):
    chips = n // CORES
    gw = group * HEAD_DIM
    cw = CORES * gw
    kw = CORES * HEAD_DIM
    tokens = n * rows
    scale = HEAD_DIM ** -0.5
    tiles = d_model // cw
    me = lax.axis_index("cp")
    chip = me // CORES
    core = me % CORES

    def peer_at(kind, src, dst, peer):
        return pltpu.make_async_remote_copy(
            src_ref=src, dst_ref=dst, send_sem=send_sem.at[kind, peer], recv_sem=recv_sem.at[kind, me],
            device_id={"cp": peer}, device_id_type=pl.DeviceIdType.MESH)

    def recv_wait(kind, dst, peer):
        pltpu.make_async_remote_copy(
            src_ref=dst, dst_ref=dst, send_sem=send_sem.at[kind, peer], recv_sem=recv_sem.at[kind, peer],
            device_id={"cp": peer}, device_id_type=pl.DeviceIdType.MESH).wait_recv()

    def rows_of(i):
        return pl.ds(pl.multiple_of(i * rows, rows), rows)

    def cols_of(i, w):
        return pl.ds(pl.multiple_of(i * w, w), w)

    def dest_chip(t):
        return (chip + gray((t + 1) % chips, chips)) % chips

    def start_parts(src, dst, sem, n_rows):
        step = n_rows // PARTS
        for i in range(PARTS):
            pltpu.make_async_copy(src.at[i * step:(i + 1) * step], dst.at[i * step:(i + 1) * step], sem).start()

    def load_kv(t):
        ch = dest_chip(t)
        a_t = wa.at[t % 2]
        start_parts(wk_hbm.at[:, cols_of(ch, kw)], a_t.at[:, 0:kw], a_sem.at[t % 2], d_model)
        start_parts(wv_hbm.at[:, cols_of(ch, kw)], a_t.at[:, kw:2 * kw], a_sem.at[t % 2], d_model)

    def load_q(t):
        start_parts(wq_hbm.at[:, cols_of(dest_chip(t), cw)], wa.at[t % 2], a_sem.at[t % 2], d_model)

    def load_do(t):
        start_parts(wo_hbm.at[cols_of(dest_chip(t), cw)], wb.at[t % 2], b_sem.at[t % 2], cw)

    def home_chip(t):
        return (chip + gray(t, chips)) % chips

    def load_y(t):
        start_parts(wo_hbm.at[cols_of(home_chip(t), cw)], wb.at[t % 2], b_sem.at[t % 2], cw)

    def load_dxq(t):
        start_parts(wq_hbm.at[:, cols_of(home_chip(t), cw)], wa.at[t % 2], a_sem.at[t % 2], d_model)

    def load_dxkv(t):
        a_t = wa.at[t % 2]
        start_parts(wk_hbm.at[:, cols_of(home_chip(t), kw)], a_t.at[:, 0:kw], a_sem.at[t % 2], d_model)
        start_parts(wv_hbm.at[:, cols_of(home_chip(t), kw)], a_t.at[:, kw:2 * kw], a_sem.at[t % 2], d_model)

    def wait_on(ref, sem):
        pltpu.make_async_copy(ref, ref, sem).wait()

    pltpu.make_async_copy(x_hbm, x_v, in_sem.at[0]).start()
    load_kv(0)
    load_kv(1)

    barrier = pltpu.get_barrier_semaphore()
    for r in range(1, n):
        pl.semaphore_signal(barrier, inc=1, device_id={"cp": (me + r) % n}, device_id_type=pl.DeviceIdType.MESH)
    pl.semaphore_wait(barrier, n - 1)

    wait_on(x_v, in_sem.at[0])

    def kv_step(t, carry):
        ch = dest_chip(t)
        wait_on(wa.at[t % 2, :, 0:2 * kw], a_sem.at[t % 2])
        res = dot_nn(x_v[...], wa[t % 2, :, 0:2 * kw]).astype(jnp.bfloat16)
        for c in range(CORES):
            kv_s[ch * CORES + c, :, 0:HEAD_DIM] = res[:, c * HEAD_DIM:(c + 1) * HEAD_DIM]
            kv_s[ch * CORES + c, :, HEAD_DIM:2 * HEAD_DIM] = res[:, kw + c * HEAD_DIM:kw + (c + 1) * HEAD_DIM]

        @pl.when(t + 2 < chips)
        def _():
            load_kv(t + 2)

        @pl.when(t + 2 >= chips)
        def _():
            load_q(t + 2 - chips)

        @pl.when(t == 0)
        def _():
            pltpu.make_async_copy(dy_hbm, dy_v, in_sem.at[1]).start()

        @pl.when((t > 0) & (t < 3))
        def _():
            load_do(t - 1)

        for c in range(CORES):
            peer = ch * CORES + (core + c) % CORES

            @pl.when(peer != me)
            def _():
                peer_at(M_KV, kv_s.at[peer], kv_r.at[rows_of(me)], peer).start()
        return carry

    lax.fori_loop(0, chips, kv_step, 0)
    wait_on(dy_v, in_sem.at[1])

    def send_heads(kind, stage, dest, ch):
        for c in range(CORES):
            peer = ch * CORES + (core + c) % CORES

            @pl.when(peer != me)
            def _():
                peer_at(kind, stage.at[peer], dest.at[rows_of(me)], peer).start()

    def qdo_step(t, carry):
        ch = dest_chip(t)
        wait_on(wa.at[t % 2], a_sem.at[t % 2])
        for i in range(cw // rows):
            res = dot_nn(x_v[...], wa[t % 2, :, i * rows:(i + 1) * rows]).astype(jnp.bfloat16)
            for j in range(rows // HEAD_DIM):
                place = i * (rows // HEAD_DIM) + j
                q_s[ch * CORES + place // group, :, (place % group) * HEAD_DIM:(place % group + 1) * HEAD_DIM] = res[:, j * HEAD_DIM:(j + 1) * HEAD_DIM]

        @pl.when(t + 2 < chips)
        def _():
            load_q(t + 2)

        @pl.when(t + 2 >= chips)
        def _():
            load_dxq(t + 2 - chips)

        send_heads(M_Q, q_s, q_r, ch)
        wait_on(wb.at[t % 2], b_sem.at[t % 2])
        for i in range(cw // rows):
            res = dot_nt(dy_v[...], wb[t % 2, i * rows:(i + 1) * rows, :]).astype(jnp.bfloat16)
            for j in range(rows // HEAD_DIM):
                place = i * (rows // HEAD_DIM) + j
                do_s[ch * CORES + place // group, :, (place % group) * HEAD_DIM:(place % group + 1) * HEAD_DIM] = res[:, j * HEAD_DIM:(j + 1) * HEAD_DIM]

        @pl.when(t + 2 < chips)
        def _():
            load_do(t + 2)

        @pl.when(t + 2 >= chips)
        def _():
            load_y(t + 2 - chips)

        send_heads(M_DO, do_s, do_r, ch)
        return carry

    lax.fori_loop(0, chips, qdo_step, 0)

    kv_r[rows_of(me), :] = kv_s[me]
    q_r[rows_of(me), :] = q_s[me]
    do_r[rows_of(me), :] = do_s[me]
    dk_v[...] = jnp.zeros_like(dk_v)
    dv_v[...] = jnp.zeros_like(dv_v)

    for r in range(1, n):
        src = (me + r) % n
        recv_wait(M_KV, kv_r.at[rows_of(src)], src)

    def turn(j, carry):
        kt[:, cols_of(j, rows)] = kv_r[rows_of(j), 0:HEAD_DIM].T
        vt[:, cols_of(j, rows)] = kv_r[rows_of(j), HEAD_DIM:2 * HEAD_DIM].T
        return carry

    lax.fori_loop(0, n, turn, 0)

    kk = scale * LOG2E
    chunks = [slice(i * CHUNK, (i + 1) * CHUNK) for i in range(tokens // CHUNK)]
    k_cols, v_cols = slice(0, HEAD_DIM), slice(HEAD_DIM, 2 * HEAD_DIM)

    def source(k):
        if chips != 4:
            c_off, o_off = k // CORES, k % CORES
        else:
            near = ((k + 2) // 4) % 2
            c_off = near * (1 + 2 * (k % 2)) + 2 * (k // 6)
            o_off = near * (k // 4) + (1 - near) * (k % 2)
        return ((chip - c_off + chips) % chips) * CORES + (core + o_off) % CORES

    def by_eights(value):
        return value.reshape(value.shape[0] // 8, 8, value.shape[1])

    def score_steps(k, probs):
        src = source(k)
        for g in range(group):
            s_ref = s_v.at[g % 2]
            st = {}

            def first(g=g, st=st):
                st["q_t"] = q_r[rows_of(src), g * HEAD_DIM:(g + 1) * HEAD_DIM].T
                st["top"] = None

            def product(sl, s_ref=s_ref, st=st):
                s_i = dot_nn(kv_r[sl, k_cols], st["q_t"])
                s_ref[sl, :] = s_i
                top = jnp.max(by_eights(s_i), axis=0)
                st["top"] = top if st["top"] is None else jnp.maximum(st["top"], top)

            def shift(st=st):
                st["mk"] = jnp.max(st["top"], axis=0, keepdims=True) * kk
                st["sum"] = None

            def add(sl, s_ref=s_ref, st=st):
                part = jnp.sum(by_eights(jnp.exp2(s_ref[sl, :] * kk - st["mk"])), axis=0)
                st["sum"] = part if st["sum"] is None else st["sum"] + part

            def close(st=st):
                st["lse"] = st["mk"] + jnp.log2(jnp.sum(st["sum"], axis=0, keepdims=True))

            def emit(sl, g=g, s_ref=s_ref, st=st):
                probs[g, sl, :] = jnp.exp2(s_ref[sl, :] * kk - st["lse"]).astype(jnp.bfloat16)

            yield 1, first
            for sl in chunks:
                yield 6, functools.partial(product, sl)
            yield 1, shift
            for sl in chunks:
                yield 6, functools.partial(add, sl)
            yield 1, close
            for sl in chunks:
                yield 6, functools.partial(emit, sl)

    def grad_steps(k, probs):
        src = source(k)
        for g in range(group):
            st = {}
            head = slice(g * HEAD_DIM, (g + 1) * HEAD_DIM)

            def outputs(g=g, head=head, st=st):
                do_t = do_r[rows_of(src), head].T
                o_t = dot_nn(vt[...], probs[g]).astype(jnp.bfloat16)
                o_s[rows_of(src), head] = o_t.T
                st["do_t"] = do_t
                st["delta"] = jnp.sum(do_t.astype(jnp.float32) * o_t.astype(jnp.float32), axis=0, keepdims=True)

            def dscore(sl, g=g, st=st):
                dp = dot_nn(kv_r[sl, v_cols], st["do_t"])
                ds_v[g, sl, :] = (probs[g, sl, :].astype(jnp.float32) * (dp - st["delta"])).astype(jnp.bfloat16)

            def dquery(g=g, head=head):
                dq_t = (dot_nn(kt[...], ds_v[g]) * scale).astype(jnp.bfloat16)
                dq_s[rows_of(src), head] = dq_t.T

            yield 12, outputs
            for sl in chunks:
                yield 4, functools.partial(dscore, sl)
            yield 10, dquery

        def accumulate(acc, left, right_ref, sl):
            total = acc[sl, :]
            part = None
            for g in range(group):
                term = dot_nn(left[g, sl, :], right_ref[rows_of(src), g * HEAD_DIM:(g + 1) * HEAD_DIM])
                part = term if part is None else part + term
            acc[sl, :] = total + part

        for sl in chunks:
            yield 12, functools.partial(accumulate, dv_v, probs, do_r, sl)
        for sl in chunks:
            yield 12, functools.partial(accumulate, dk_v, ds_v, q_r, sl)

    def run_steps(*streams):
        lists = [list(s) for s in streams]
        totals = [sum(w for w, _ in s) for s in lists]
        tagged = []
        for order, (steps, whole) in enumerate(zip(lists, totals)):
            at = 0
            for w, f in steps:
                tagged.append(((at + w / 2) / whole, order, len(tagged), f))
                at += w
        for _, _, _, f in sorted(tagged, key=lambda t: t[:3]):
            f()

    def need(kind, dest, k):
        src = source(k)

        @pl.when((k > 0) & (k < n))
        def _():
            recv_wait(kind, dest.at[rows_of(src)], src)


    def attend(k, carry):
        need(M_Q, q_r, k)
        need(M_DO, do_r, k)
        run_steps(score_steps(k, p_v.at[0])); run_steps(grad_steps(k, p_v.at[0]))
        src = source(k)

        @pl.when(k > 0)
        def _():
            peer_at(M_O, o_s.at[rows_of(src)], o_r.at[:, cols_of(me, gw)], src).start()
            peer_at(M_DQ, dq_s.at[rows_of(src)], dq_r.at[:, cols_of(me, gw)], src).start()
        return carry

    lax.fori_loop(0, n, attend, 0)

    def dk_place(owner, which):
        return cols_of((owner // CORES) * 2 * CORES + which * CORES + owner % CORES, HEAD_DIM)

    def finish(j, carry):
        dst = ((chip + gray(chips - 1 - j // CORES, chips)) % chips) * CORES + (core + 1 + j % CORES) % CORES
        dk_s[dst] = (dk_v[rows_of(dst), :] * scale).astype(jnp.bfloat16)
        dv_s[dst] = dv_v[rows_of(dst), :].astype(jnp.bfloat16)

        @pl.when(dst != me)
        def _():
            peer_at(M_DK, dk_s.at[dst], dkv_r.at[:, dk_place(me, 0)], dst).start()
            peer_at(M_DV, dv_s.at[dst], dkv_r.at[:, dk_place(me, 1)], dst).start()
        return carry

    lax.fori_loop(0, n, finish, 0)

    o_r[:, cols_of(me, gw)] = o_s[rows_of(me), :]
    dq_r[:, cols_of(me, gw)] = dq_s[rows_of(me), :]
    dkv_r[:, dk_place(me, 0)] = dk_s[me]
    dkv_r[:, dk_place(me, 1)] = dv_s[me]
    pieces = d_model // rows
    y_acc[...] = jnp.zeros_like(y_acc)

    def dx_ref(c):
        return s_v.at[c // n, (c % n) * rows:(c % n + 1) * rows, :]

    for c in range(pieces):
        dx_ref(c)[...] = jnp.zeros((rows, rows), jnp.float32)

    def from_chip(t, wait):
        for c in range(CORES):
            src = home_chip(t) * CORES + (core + 1 + c) % CORES

            @pl.when(src != me)
            def _():
                wait(src)

    def wait_dkv(src):
        recv_wait(M_DK, dkv_r.at[:, dk_place(src, 0)], src)
        recv_wait(M_DV, dkv_r.at[:, dk_place(src, 1)], src)

    def back_step(t, carry):
        ch = home_chip(t)
        wait_on(wb.at[t % 2], b_sem.at[t % 2])
        from_chip(t, lambda src: recv_wait(M_O, o_r.at[:, cols_of(src, gw)], src))
        left = o_r[:, cols_of(ch, cw)]
        for c in range(pieces // PIECE):
            sl = slice(c * PIECE * rows, (c + 1) * PIECE * rows)
            y_acc[:, sl] += dot_nn(left, wb[t % 2, :, sl])

        @pl.when(t + 2 < chips)
        def _():
            load_y(t + 2)

        wait_on(wa.at[t % 2], a_sem.at[t % 2])
        from_chip(t, lambda src: recv_wait(M_DQ, dq_r.at[:, cols_of(src, gw)], src))
        left = dq_r[:, cols_of(ch, cw)]
        for c in range(pieces):
            dx_ref(c)[...] += dot_nt(left, wa[t % 2, c * rows:(c + 1) * rows, :])

        @pl.when(t + 2 < chips)
        def _():
            load_dxq(t + 2)

        @pl.when(t + 2 >= chips)
        def _():
            load_dxkv(t + 2 - chips)
        return carry

    lax.fori_loop(0, chips, back_step, 0)

    def put_out(i, hbm, value):
        if i >= 2:
            wait_on(out_v.at[i % 2], out_sem.at[i % 2])
        out_v[i % 2] = value
        pltpu.make_async_copy(out_v.at[i % 2], hbm.at[:, i * cw:(i + 1) * cw], out_sem.at[i % 2]).start()

    def drain_out():
        for i in range(2):
            wait_on(out_v.at[i], out_sem.at[i])

    for i in range(tiles):
        put_out(i, y_hbm, y_acc[:, i * cw:(i + 1) * cw].astype(jnp.bfloat16))

    def dxkv_step(t, carry):
        ch = home_chip(t)
        wait_on(wa.at[t % 2, :, 0:2 * kw], a_sem.at[t % 2])
        from_chip(t, wait_dkv)
        left = dkv_r[:, cols_of(ch, 2 * kw)]
        for c in range(pieces):
            dx_ref(c)[...] += dot_nt(left, wa[t % 2, c * rows:(c + 1) * rows, 0:2 * kw])

        @pl.when(t + 2 < chips)
        def _():
            load_dxkv(t + 2)
        return carry

    lax.fori_loop(0, chips, dxkv_step, 0)
    drain_out()
    for i in range(tiles):
        each = cw // rows
        value = jnp.concatenate([dx_ref(i * each + c)[...] for c in range(each)], axis=1)
        put_out(i, dx_hbm, value.astype(jnp.bfloat16))
    drain_out()

    for r in range(1, n):
        peer = (me + r) % n
        peer_at(M_KV, kv_s.at[peer], kv_r.at[rows_of(me)], peer).wait_send()
        peer_at(M_Q, q_s.at[peer], q_r.at[rows_of(me)], peer).wait_send()
        peer_at(M_DO, do_s.at[peer], do_r.at[rows_of(me)], peer).wait_send()
        peer_at(M_O, o_s.at[rows_of(peer)], o_r.at[:, cols_of(me, gw)], peer).wait_send()
        peer_at(M_DQ, dq_s.at[rows_of(peer)], dq_r.at[:, cols_of(me, gw)], peer).wait_send()
        peer_at(M_DK, dk_s.at[peer], dkv_r.at[:, dk_place(me, 0)], peer).wait_send()
        peer_at(M_DV, dv_s.at[peer], dkv_r.at[:, dk_place(me, 1)], peer).wait_send()


def solution(mesh):
    n = mesh.shape["cp"]
    row_spec = P(("dp", "cp"), None)
    full_spec = P(None, None)

    def local_body(x_loc, dy_loc, w_q, w_k, w_v, w_o):
        rows, d_model = x_loc.shape
        q_heads = w_q.shape[1] // HEAD_DIM
        kv_heads = w_k.shape[1] // HEAD_DIM
        group = q_heads // kv_heads
        assert kv_heads == n and n % CORES == 0
        gw = group * HEAD_DIM
        cw = CORES * gw
        assert q_heads * HEAD_DIM == d_model and d_model % rows == 0 and d_model // rows <= 2 * n
        tokens = n * rows
        bf, f32 = jnp.bfloat16, jnp.float32
        vm = pltpu.VMEM
        scratch = [
            vm((rows, d_model), bf), vm((rows, d_model), bf),
            vm((2, d_model, cw), bf), vm((2, cw, d_model), bf),
            vm((n, rows, 2 * HEAD_DIM), bf), vm((n, rows, gw), bf), vm((n, rows, gw), bf),
            vm((tokens, 2 * HEAD_DIM), bf), vm((tokens, gw), bf), vm((tokens, gw), bf),
            vm((HEAD_DIM, tokens), bf), vm((HEAD_DIM, tokens), bf),
            vm((tokens, gw), bf), vm((tokens, gw), bf),
            vm((rows, n * gw), bf), vm((rows, n * gw), bf),
            vm((tokens, HEAD_DIM), f32), vm((tokens, HEAD_DIM), f32),
            vm((n, rows, HEAD_DIM), bf), vm((n, rows, HEAD_DIM), bf),
            vm((rows, 2 * n * HEAD_DIM), bf),
            vm((2, tokens, rows), f32),
            vm((1, group, tokens, rows), bf), vm((group, tokens, rows), bf),
            vm((rows, d_model), f32), vm((2, rows, cw), bf),
            pltpu.SemaphoreType.DMA((2,)), pltpu.SemaphoreType.DMA((2,)), pltpu.SemaphoreType.DMA((2,)),
            pltpu.SemaphoreType.DMA((2,)),
            pltpu.SemaphoreType.DMA((N_KINDS, n)), pltpu.SemaphoreType.DMA((N_KINDS, n)),
        ]
        out = jax.ShapeDtypeStruct((rows, d_model), bf)
        return pl.pallas_call(
            functools.partial(body, n, rows, d_model, group),
            out_shape=(out, out),
            in_specs=[pl.BlockSpec(memory_space=pl.ANY)] * 6,
            out_specs=(pl.BlockSpec(memory_space=pl.ANY), pl.BlockSpec(memory_space=pl.ANY)),
            scratch_shapes=scratch,
            compiler_params=pltpu.CompilerParams(collective_id=0, has_side_effects=True,
                                                 vmem_limit_bytes=63 * 1024 * 1024),
        )(x_loc, dy_loc, w_q, w_k, w_v, w_o)

    return jax.shard_map(local_body, mesh=mesh,
                         in_specs=(row_spec, row_spec, full_spec, full_spec, full_spec, full_spec),
                         out_specs=(row_spec, row_spec), check_vma=False)
```

```python
import functools

import jax
import jax.numpy as jnp
from jax import lax
from jax.experimental import pallas as pl
from jax.experimental.pallas import tpu as pltpu
from jax.sharding import PartitionSpec as P

HEAD_DIM = 128
CORES = 2
LOG2E = 1.4426950408889634
M_KV, M_Q, M_DO, M_O, M_DQ, M_DK, M_DV = range(7)
N_KINDS = 7
PARTS = 4
PIECE = 1
CHUNK = 1024


def gray(q, n_chips):
    if n_chips != 4:
        return q
    return q + (q // 2) * (1 - 2 * (q % 2))


def dot_nn(a, b):
    return lax.dot_general(a, b, (((1,), (0,)), ((), ())), preferred_element_type=jnp.float32)


def dot_nt(a, b):
    return lax.dot_general(a, b, (((1,), (1,)), ((), ())), preferred_element_type=jnp.float32)


def body(n, rows, d_model, group,
         x_hbm, dy_hbm, wq_hbm, wk_hbm, wv_hbm, wo_hbm,
         y_hbm, dx_hbm,
         x_v, dy_v, wa, wb, kv_s, q_s, do_s, kv_r, q_r, do_r, kt, vt,
         o_s, dq_s, o_r, dq_r, dk_v, dv_v, dk_s, dv_s, dkv_r,
         s_v, p_v, ds_v, y_acc, out_v,
         in_sem, a_sem, b_sem, out_sem, send_sem, recv_sem):
    chips = n // CORES
    gw = group * HEAD_DIM
    cw = CORES * gw
    kw = CORES * HEAD_DIM
    tokens = n * rows
    scale = HEAD_DIM ** -0.5
    tiles = d_model // cw
    me = lax.axis_index("cp")
    chip = me // CORES
    core = me % CORES

    def peer_at(kind, src, dst, peer):
        return pltpu.make_async_remote_copy(
            src_ref=src, dst_ref=dst, send_sem=send_sem.at[kind, peer], recv_sem=recv_sem.at[kind, me],
            device_id={"cp": peer}, device_id_type=pl.DeviceIdType.MESH)

    def recv_wait(kind, dst, peer):
        pltpu.make_async_remote_copy(
            src_ref=dst, dst_ref=dst, send_sem=send_sem.at[kind, peer], recv_sem=recv_sem.at[kind, peer],
            device_id={"cp": peer}, device_id_type=pl.DeviceIdType.MESH).wait_recv()

    def rows_of(i):
        return pl.ds(pl.multiple_of(i * rows, rows), rows)

    def cols_of(i, w):
        return pl.ds(pl.multiple_of(i * w, w), w)

    def dest_chip(t):
        return (chip + gray(chips - 1 - t, chips)) % chips

    def start_parts(src, dst, sem, n_rows):
        step = n_rows // PARTS
        for i in range(PARTS):
            pltpu.make_async_copy(src.at[i * step:(i + 1) * step], dst.at[i * step:(i + 1) * step], sem).start()

    def load_kv(t):
        ch = dest_chip(t)
        a_t = wa.at[t % 2]
        start_parts(wk_hbm.at[:, cols_of(ch, kw)], a_t.at[:, 0:kw], a_sem.at[t % 2], d_model)
        start_parts(wv_hbm.at[:, cols_of(ch, kw)], a_t.at[:, kw:2 * kw], a_sem.at[t % 2], d_model)

    def load_q(t):
        start_parts(wq_hbm.at[:, cols_of(dest_chip(t), cw)], wa.at[t % 2], a_sem.at[t % 2], d_model)

    def load_do(t):
        start_parts(wo_hbm.at[cols_of(dest_chip(t), cw)], wb.at[t % 2], b_sem.at[t % 2], cw)

    def home_chip(t):
        return (chip + gray((chips - t) % chips, chips)) % chips

    def load_y(t):
        start_parts(wo_hbm.at[cols_of(home_chip(t), cw)], wb.at[t % 2], b_sem.at[t % 2], cw)

    def load_dxq(t):
        start_parts(wq_hbm.at[:, cols_of(home_chip(t), cw)], wa.at[t % 2], a_sem.at[t % 2], d_model)

    def load_dxkv(t):
        a_t = wa.at[t % 2]
        start_parts(wk_hbm.at[:, cols_of(home_chip(t), kw)], a_t.at[:, 0:kw], a_sem.at[t % 2], d_model)
        start_parts(wv_hbm.at[:, cols_of(home_chip(t), kw)], a_t.at[:, kw:2 * kw], a_sem.at[t % 2], d_model)

    def wait_on(ref, sem):
        pltpu.make_async_copy(ref, ref, sem).wait()

    pltpu.make_async_copy(x_hbm, x_v, in_sem.at[0]).start()
    load_kv(0)

    barrier = pltpu.get_barrier_semaphore()
    for r in range(1, n):
        pl.semaphore_signal(barrier, inc=1, device_id={"cp": (me + r) % n}, device_id_type=pl.DeviceIdType.MESH)
    load_kv(1)
    pl.semaphore_wait(barrier, n - 1)

    wait_on(x_v, in_sem.at[0])

    def kv_step(t, carry):
        ch = dest_chip(t)
        wait_on(wa.at[t % 2, :, 0:2 * kw], a_sem.at[t % 2])
        res = dot_nn(x_v[...], wa[t % 2, :, 0:2 * kw]).astype(jnp.bfloat16)
        for c in range(CORES):
            kv_s[ch * CORES + c, :, 0:HEAD_DIM] = res[:, c * HEAD_DIM:(c + 1) * HEAD_DIM]
            kv_s[ch * CORES + c, :, HEAD_DIM:2 * HEAD_DIM] = res[:, kw + c * HEAD_DIM:kw + (c + 1) * HEAD_DIM]

        @pl.when(t + 2 < chips)
        def _():
            load_kv(t + 2)

        @pl.when(t + 2 >= chips)
        def _():
            load_q(t + 2 - chips)

        @pl.when(t == 0)
        def _():
            pltpu.make_async_copy(dy_hbm, dy_v, in_sem.at[1]).start()

        @pl.when((t > 0) & (t < 3))
        def _():
            load_do(t - 1)

        for c in range(CORES):
            peer = ch * CORES + (core + c) % CORES

            @pl.when(peer != me)
            def _():
                peer_at(M_KV, kv_s.at[peer], kv_r.at[rows_of(me)], peer).start()
        return carry

    lax.fori_loop(0, chips, kv_step, 0)
    wait_on(dy_v, in_sem.at[1])

    def send_heads(kind, stage, dest, ch):
        for c in range(CORES):
            peer = ch * CORES + (core + c) % CORES

            @pl.when(peer != me)
            def _():
                peer_at(kind, stage.at[peer], dest.at[rows_of(me)], peer).start()

    def qdo_step(t, carry):
        ch = dest_chip(t)
        wait_on(wa.at[t % 2], a_sem.at[t % 2])
        for i in range(cw // rows):
            res = dot_nn(x_v[...], wa[t % 2, :, i * rows:(i + 1) * rows]).astype(jnp.bfloat16)
            for j in range(rows // HEAD_DIM):
                place = i * (rows // HEAD_DIM) + j
                q_s[ch * CORES + place // group, :, (place % group) * HEAD_DIM:(place % group + 1) * HEAD_DIM] = res[:, j * HEAD_DIM:(j + 1) * HEAD_DIM]

        @pl.when(t + 2 < chips)
        def _():
            load_q(t + 2)

        @pl.when(t + 2 >= chips)
        def _():
            load_dxq(t + 2 - chips)

        send_heads(M_Q, q_s, q_r, ch)
        wait_on(wb.at[t % 2], b_sem.at[t % 2])
        for i in range(cw // rows):
            res = dot_nt(dy_v[...], wb[t % 2, i * rows:(i + 1) * rows, :]).astype(jnp.bfloat16)
            for j in range(rows // HEAD_DIM):
                place = i * (rows // HEAD_DIM) + j
                do_s[ch * CORES + place // group, :, (place % group) * HEAD_DIM:(place % group + 1) * HEAD_DIM] = res[:, j * HEAD_DIM:(j + 1) * HEAD_DIM]

        @pl.when(t + 2 < chips)
        def _():
            load_do(t + 2)

        @pl.when(t + 2 >= chips)
        def _():
            load_y(t + 2 - chips)

        send_heads(M_DO, do_s, do_r, ch)
        return carry

    lax.fori_loop(0, chips, qdo_step, 0)

    kv_r[rows_of(me), :] = kv_s[me]
    q_r[rows_of(me), :] = q_s[me]
    do_r[rows_of(me), :] = do_s[me]
    dk_v[...] = jnp.zeros_like(dk_v)
    dv_v[...] = jnp.zeros_like(dv_v)

    for r in range(1, n):
        src = (me + r) % n
        recv_wait(M_KV, kv_r.at[rows_of(src)], src)

    def turn(j, carry):
        kt[:, cols_of(j, rows)] = kv_r[rows_of(j), 0:HEAD_DIM].T
        vt[:, cols_of(j, rows)] = kv_r[rows_of(j), HEAD_DIM:2 * HEAD_DIM].T
        return carry

    lax.fori_loop(0, n, turn, 0)

    kk = scale * LOG2E
    chunks = [slice(i * CHUNK, (i + 1) * CHUNK) for i in range(tokens // CHUNK)]
    k_cols, v_cols = slice(0, HEAD_DIM), slice(HEAD_DIM, 2 * HEAD_DIM)

    def source(k):
        if chips != 4:
            c_off, o_off = (chips - k // CORES) % chips, k % CORES
        else:
            near = k // 4
            c_off = near * (3 - 2 * (k % 2)) + (1 - near) * 2 * (k // 2)
            o_off = near * (k // 2 - 2) + (1 - near) * (k % 2)
        return ((chip - c_off + chips) % chips) * CORES + (core + o_off) % CORES

    def by_eights(value):
        return value.reshape(value.shape[0] // 8, 8, value.shape[1])

    def score_steps(k, probs):
        src = source(k)
        for g in range(group):
            s_ref = s_v.at[g % 2]
            st = {}

            def first(g=g, st=st):
                st["q_t"] = q_r[rows_of(src), g * HEAD_DIM:(g + 1) * HEAD_DIM].T
                st["top"] = None

            def product(sl, s_ref=s_ref, st=st):
                s_i = dot_nn(kv_r[sl, k_cols], st["q_t"])
                s_ref[sl, :] = s_i
                top = jnp.max(by_eights(s_i), axis=0)
                st["top"] = top if st["top"] is None else jnp.maximum(st["top"], top)

            def shift(st=st):
                st["mk"] = jnp.max(st["top"], axis=0, keepdims=True) * kk
                st["sum"] = None

            def add(sl, s_ref=s_ref, st=st):
                part = jnp.sum(by_eights(jnp.exp2(s_ref[sl, :] * kk - st["mk"])), axis=0)
                st["sum"] = part if st["sum"] is None else st["sum"] + part

            def close(st=st):
                st["lse"] = st["mk"] + jnp.log2(jnp.sum(st["sum"], axis=0, keepdims=True))

            def emit(sl, g=g, s_ref=s_ref, st=st):
                probs[g, sl, :] = jnp.exp2(s_ref[sl, :] * kk - st["lse"]).astype(jnp.bfloat16)

            yield 1, first
            for sl in chunks:
                yield 6, functools.partial(product, sl)
            yield 1, shift
            for sl in chunks:
                yield 6, functools.partial(add, sl)
            yield 1, close
            for sl in chunks:
                yield 6, functools.partial(emit, sl)

    def grad_steps(k, probs):
        src = source(k)
        for g in range(group):
            st = {}
            head = slice(g * HEAD_DIM, (g + 1) * HEAD_DIM)

            def outputs(g=g, head=head, st=st):
                do_t = do_r[rows_of(src), head].T
                o_t = dot_nn(vt[...], probs[g]).astype(jnp.bfloat16)
                o_s[rows_of(src), head] = o_t.T
                st["do_t"] = do_t
                st["delta"] = jnp.sum(do_t.astype(jnp.float32) * o_t.astype(jnp.float32), axis=0, keepdims=True)

            def dscore(sl, g=g, st=st):
                dp = dot_nn(kv_r[sl, v_cols], st["do_t"])
                ds_v[g, sl, :] = (probs[g, sl, :].astype(jnp.float32) * (dp - st["delta"])).astype(jnp.bfloat16)

            def dquery(g=g, head=head):
                dq_t = (dot_nn(kt[...], ds_v[g]) * scale).astype(jnp.bfloat16)
                dq_s[rows_of(src), head] = dq_t.T

            yield 12, outputs
            for sl in chunks:
                yield 4, functools.partial(dscore, sl)
            yield 10, dquery

        def accumulate(acc, left, right_ref, sl):
            total = acc[sl, :]
            part = None
            for g in range(group):
                term = dot_nn(left[g, sl, :], right_ref[rows_of(src), g * HEAD_DIM:(g + 1) * HEAD_DIM])
                part = term if part is None else part + term
            acc[sl, :] = total + part

        for sl in chunks:
            yield 12, functools.partial(accumulate, dv_v, probs, do_r, sl)
        for sl in chunks:
            yield 12, functools.partial(accumulate, dk_v, ds_v, q_r, sl)

    def run_steps(*streams):
        lists = [list(s) for s in streams]
        totals = [sum(w for w, _ in s) for s in lists]
        tagged = []
        for order, (steps, whole) in enumerate(zip(lists, totals)):
            at = 0
            for w, f in steps:
                tagged.append(((at + w / 2) / whole, order, len(tagged), f))
                at += w
        for _, _, _, f in sorted(tagged, key=lambda t: t[:3]):
            f()

    def need(kind, dest, k):
        src = source(k)

        @pl.when((k > 0) & (k < n))
        def _():
            recv_wait(kind, dest.at[rows_of(src)], src)


    def attend(k, carry):
        need(M_Q, q_r, k)
        need(M_DO, do_r, k)
        run_steps(score_steps(k, p_v.at[0])); run_steps(grad_steps(k, p_v.at[0]))
        src = source(k)

        @pl.when(k > 0)
        def _():
            peer_at(M_O, o_s.at[rows_of(src)], o_r.at[:, cols_of(me, gw)], src).start()
            peer_at(M_DQ, dq_s.at[rows_of(src)], dq_r.at[:, cols_of(me, gw)], src).start()
        return carry

    lax.fori_loop(0, n, attend, 0)

    def dk_place(owner, which):
        return cols_of((owner // CORES) * 2 * CORES + which * CORES + owner % CORES, HEAD_DIM)

    def finish(j, carry):
        dst = ((chip + gray(chips - 1 - j // CORES, chips)) % chips) * CORES + (core + 1 + j % CORES) % CORES
        dk_s[dst] = (dk_v[rows_of(dst), :] * scale).astype(jnp.bfloat16)
        dv_s[dst] = dv_v[rows_of(dst), :].astype(jnp.bfloat16)

        @pl.when(dst != me)
        def _():
            peer_at(M_DK, dk_s.at[dst], dkv_r.at[:, dk_place(me, 0)], dst).start()
            peer_at(M_DV, dv_s.at[dst], dkv_r.at[:, dk_place(me, 1)], dst).start()
        return carry

    lax.fori_loop(0, n, finish, 0)

    o_r[:, cols_of(me, gw)] = o_s[rows_of(me), :]
    dq_r[:, cols_of(me, gw)] = dq_s[rows_of(me), :]
    dkv_r[:, dk_place(me, 0)] = dk_s[me]
    dkv_r[:, dk_place(me, 1)] = dv_s[me]
    pieces = d_model // rows
    y_acc[...] = jnp.zeros_like(y_acc)

    def dx_ref(c):
        return s_v.at[c // n, (c % n) * rows:(c % n + 1) * rows, :]

    for c in range(pieces):
        dx_ref(c)[...] = jnp.zeros((rows, rows), jnp.float32)

    def from_chip(t, wait):
        for c in range(CORES):
            src = home_chip(t) * CORES + (core + 1 + c) % CORES

            @pl.when(src != me)
            def _():
                wait(src)

    def wait_dkv(src):
        recv_wait(M_DK, dkv_r.at[:, dk_place(src, 0)], src)
        recv_wait(M_DV, dkv_r.at[:, dk_place(src, 1)], src)

    def back_step(t, carry):
        ch = home_chip(t)
        wait_on(wb.at[t % 2], b_sem.at[t % 2])
        from_chip(t, lambda src: recv_wait(M_O, o_r.at[:, cols_of(src, gw)], src))
        left = o_r[:, cols_of(ch, cw)]
        for c in range(pieces // PIECE):
            sl = slice(c * PIECE * rows, (c + 1) * PIECE * rows)
            y_acc[:, sl] += dot_nn(left, wb[t % 2, :, sl])

        @pl.when(t + 2 < chips)
        def _():
            load_y(t + 2)

        wait_on(wa.at[t % 2], a_sem.at[t % 2])
        from_chip(t, lambda src: recv_wait(M_DQ, dq_r.at[:, cols_of(src, gw)], src))
        left = dq_r[:, cols_of(ch, cw)]
        for c in range(pieces):
            dx_ref(c)[...] += dot_nt(left, wa[t % 2, c * rows:(c + 1) * rows, :])

        @pl.when(t + 2 < chips)
        def _():
            load_dxq(t + 2)

        @pl.when(t + 2 >= chips)
        def _():
            load_dxkv(t + 2 - chips)
        return carry

    lax.fori_loop(0, chips, back_step, 0)

    def put_out(i, hbm, value):
        out_v[i] = value
        pltpu.make_async_copy(out_v.at[i], hbm.at[:, i * cw:(i + 1) * cw], out_sem.at[i % 2]).start()

    def drain_out():
        for i in range(2):
            wait_on(out_v.at[0:tiles // 2], out_sem.at[i])

    for i in range(tiles):
        put_out(i, y_hbm, y_acc[:, i * cw:(i + 1) * cw].astype(jnp.bfloat16))

    def dxkv_step(t, carry):
        ch = home_chip(t)
        wait_on(wa.at[t % 2, :, 0:2 * kw], a_sem.at[t % 2])
        from_chip(t, wait_dkv)
        left = dkv_r[:, cols_of(ch, 2 * kw)]
        for c in range(pieces):
            dx_ref(c)[...] += dot_nt(left, wa[t % 2, c * rows:(c + 1) * rows, 0:2 * kw])

        @pl.when(t + 2 < chips)
        def _():
            load_dxkv(t + 2)
        return carry

    lax.fori_loop(0, chips - 1, dxkv_step, 0)
    drain_out()
    last = chips - 1
    wait_on(wa.at[last % 2, :, 0:2 * kw], a_sem.at[last % 2])
    from_chip(last, wait_dkv)
    left = dkv_r[:, cols_of(home_chip(last), 2 * kw)]
    each = cw // rows
    for i in range(tiles):
        done = []
        for c in range(i * each, (i + 1) * each):
            done.append(dx_ref(c)[...] + dot_nt(left, wa[last % 2, c * rows:(c + 1) * rows, 0:2 * kw]))
        out_v[i] = jnp.concatenate(done, axis=1).astype(jnp.bfloat16)
    for i in range(tiles):
        pltpu.make_async_copy(out_v.at[i], dx_hbm.at[:, i * cw:(i + 1) * cw], out_sem.at[i % 2]).start()
    drain_out()

    for r in range(1, n):
        peer = (me + r) % n
        peer_at(M_KV, kv_s.at[peer], kv_r.at[rows_of(me)], peer).wait_send()
        peer_at(M_Q, q_s.at[peer], q_r.at[rows_of(me)], peer).wait_send()
        peer_at(M_DO, do_s.at[peer], do_r.at[rows_of(me)], peer).wait_send()
        peer_at(M_O, o_s.at[rows_of(peer)], o_r.at[:, cols_of(me, gw)], peer).wait_send()
        peer_at(M_DQ, dq_s.at[rows_of(peer)], dq_r.at[:, cols_of(me, gw)], peer).wait_send()
        peer_at(M_DK, dk_s.at[peer], dkv_r.at[:, dk_place(me, 0)], peer).wait_send()
        peer_at(M_DV, dv_s.at[peer], dkv_r.at[:, dk_place(me, 1)], peer).wait_send()


def solution(mesh):
    n = mesh.shape["cp"]
    row_spec = P(("dp", "cp"), None)
    full_spec = P(None, None)

    def local_body(x_loc, dy_loc, w_q, w_k, w_v, w_o):
        rows, d_model = x_loc.shape
        q_heads = w_q.shape[1] // HEAD_DIM
        kv_heads = w_k.shape[1] // HEAD_DIM
        group = q_heads // kv_heads
        assert kv_heads == n and n % CORES == 0
        gw = group * HEAD_DIM
        cw = CORES * gw
        assert q_heads * HEAD_DIM == d_model and d_model % rows == 0 and d_model // rows <= 2 * n and d_model % (2 * cw) == 0
        tokens = n * rows
        bf, f32 = jnp.bfloat16, jnp.float32
        vm = pltpu.VMEM
        scratch = [
            vm((rows, d_model), bf), vm((rows, d_model), bf),
            vm((2, d_model, cw), bf), vm((2, cw, d_model), bf),
            vm((n, rows, 2 * HEAD_DIM), bf), vm((n, rows, gw), bf), vm((n, rows, gw), bf),
            vm((tokens, 2 * HEAD_DIM), bf), vm((tokens, gw), bf), vm((tokens, gw), bf),
            vm((HEAD_DIM, tokens), bf), vm((HEAD_DIM, tokens), bf),
            vm((tokens, gw), bf), vm((tokens, gw), bf),
            vm((rows, n * gw), bf), vm((rows, n * gw), bf),
            vm((tokens, HEAD_DIM), f32), vm((tokens, HEAD_DIM), f32),
            vm((n, rows, HEAD_DIM), bf), vm((n, rows, HEAD_DIM), bf),
            vm((rows, 2 * n * HEAD_DIM), bf),
            vm((2, tokens, rows), f32),
            vm((1, group, tokens, rows), bf), vm((group, tokens, rows), bf),
            vm((rows, d_model), f32), vm((d_model // cw, rows, cw), bf),
            pltpu.SemaphoreType.DMA((2,)), pltpu.SemaphoreType.DMA((2,)), pltpu.SemaphoreType.DMA((2,)),
            pltpu.SemaphoreType.DMA((2,)),
            pltpu.SemaphoreType.DMA((N_KINDS, n)), pltpu.SemaphoreType.DMA((N_KINDS, n)),
        ]
        out = jax.ShapeDtypeStruct((rows, d_model), bf)
        return pl.pallas_call(
            functools.partial(body, n, rows, d_model, group),
            out_shape=(out, out),
            in_specs=[pl.BlockSpec(memory_space=pl.ANY)] * 6,
            out_specs=(pl.BlockSpec(memory_space=pl.ANY), pl.BlockSpec(memory_space=pl.ANY)),
            scratch_shapes=scratch,
            compiler_params=pltpu.CompilerParams(collective_id=0, has_side_effects=True,
                                                 vmem_limit_bytes=63 * 1024 * 1024),
        )(x_loc, dy_loc, w_q, w_k, w_v, w_o)

    return jax.shard_map(local_body, mesh=mesh,
                         in_specs=(row_spec, row_spec, full_spec, full_spec, full_spec, full_spec),
                         out_specs=(row_spec, row_spec), check_vma=False)
```

```python
import functools

import jax
import jax.numpy as jnp
from jax import lax
from jax.experimental import pallas as pl
from jax.experimental.pallas import tpu as pltpu
from jax.sharding import PartitionSpec as P

HEAD_DIM = 128
CORES = 2
LOG2E = 1.4426950408889634
M_KV, M_Q, M_DO, M_O, M_DQ, M_DK, M_DV = range(7)
N_KINDS = 7
PARTS = 4
PIECE = 1
CHUNK = 1024


def gray(q, n_chips):
    if n_chips != 4:
        return q
    return q + (q // 2) * (1 - 2 * (q % 2))


def dot_nn(a, b):
    return lax.dot_general(a, b, (((1,), (0,)), ((), ())), preferred_element_type=jnp.float32)


def dot_nt(a, b):
    return lax.dot_general(a, b, (((1,), (1,)), ((), ())), preferred_element_type=jnp.float32)


def body(n, rows, d_model, group,
         x_hbm, dy_hbm, wq_hbm, wk_hbm, wv_hbm, wo_hbm,
         y_out, dx_out,
         x_v, dy_v, wa, wb, kv_s, q_s, do_s, kv_r, q_r, do_r, kt, vt,
         o_s, dq_s, o_r, dq_r, dk_v, dv_v, dkv_r,
         s_v, p_v, ds_v, y_acc,
         in_sem, a_sem, b_sem, send_sem, recv_sem):
    chips = n // CORES
    gw = group * HEAD_DIM
    cw = CORES * gw
    kw = CORES * HEAD_DIM
    tokens = n * rows
    scale = HEAD_DIM ** -0.5
    tiles = d_model // cw
    me = lax.axis_index("cp")
    chip = me // CORES
    core = me % CORES

    def peer_at(kind, src, dst, peer):
        return pltpu.make_async_remote_copy(
            src_ref=src, dst_ref=dst, send_sem=send_sem.at[kind, peer], recv_sem=recv_sem.at[kind, me],
            device_id={"cp": peer}, device_id_type=pl.DeviceIdType.MESH)

    def recv_wait(kind, dst, peer):
        pltpu.make_async_remote_copy(
            src_ref=dst, dst_ref=dst, send_sem=send_sem.at[kind, peer], recv_sem=recv_sem.at[kind, peer],
            device_id={"cp": peer}, device_id_type=pl.DeviceIdType.MESH).wait_recv()

    def rows_of(i):
        return pl.ds(pl.multiple_of(i * rows, rows), rows)

    def cols_of(i, w):
        return pl.ds(pl.multiple_of(i * w, w), w)

    def dest_chip(t):
        return (chip + gray(chips - 1 - t, chips)) % chips

    def start_parts(src, dst, sem, n_rows):
        step = n_rows // PARTS
        for i in range(PARTS):
            pltpu.make_async_copy(src.at[i * step:(i + 1) * step], dst.at[i * step:(i + 1) * step], sem).start()

    def load_kv(t):
        ch = dest_chip(t)
        a_t = wa.at[t % 2]
        start_parts(wk_hbm.at[:, cols_of(ch, kw)], a_t.at[:, 0:kw], a_sem.at[t % 2], d_model)
        start_parts(wv_hbm.at[:, cols_of(ch, kw)], a_t.at[:, kw:2 * kw], a_sem.at[t % 2], d_model)

    def load_q(t):
        start_parts(wq_hbm.at[:, cols_of(dest_chip(t), cw)], wa.at[t % 2], a_sem.at[t % 2], d_model)

    def load_do(t):
        start_parts(wo_hbm.at[cols_of(dest_chip(t), cw)], wb.at[t % 2], b_sem.at[t % 2], cw)

    def home_chip(t):
        return (chip + gray((chips - t) % chips, chips)) % chips

    def load_y(t):
        start_parts(wo_hbm.at[cols_of(home_chip(t), cw)], wb.at[t % 2], b_sem.at[t % 2], cw)

    def load_dxq(t):
        start_parts(wq_hbm.at[:, cols_of(home_chip(t), cw)], wa.at[t % 2], a_sem.at[t % 2], d_model)

    def load_dxkv(t):
        a_t = wa.at[t % 2]
        start_parts(wk_hbm.at[:, cols_of(home_chip(t), kw)], a_t.at[:, 0:kw], a_sem.at[t % 2], d_model)
        start_parts(wv_hbm.at[:, cols_of(home_chip(t), kw)], a_t.at[:, kw:2 * kw], a_sem.at[t % 2], d_model)

    def wait_on(ref, sem):
        pltpu.make_async_copy(ref, ref, sem).wait()

    pltpu.make_async_copy(x_hbm, x_v, in_sem.at[0]).start()
    load_kv(0)

    barrier = pltpu.get_barrier_semaphore()
    for r in range(1, n):
        pl.semaphore_signal(barrier, inc=1, device_id={"cp": (me + r) % n}, device_id_type=pl.DeviceIdType.MESH)
    load_kv(1)

    wait_on(x_v, in_sem.at[0])

    def kv_step(t, carry, first=False):
        ch = dest_chip(t)
        wait_on(wa.at[t % 2, :, 0:2 * kw], a_sem.at[t % 2])
        res = dot_nn(x_v[...], wa[t % 2, :, 0:2 * kw]).astype(jnp.bfloat16)
        for c in range(CORES):
            kv_s[ch * CORES + c, :, 0:HEAD_DIM] = res[:, c * HEAD_DIM:(c + 1) * HEAD_DIM]
            kv_s[ch * CORES + c, :, HEAD_DIM:2 * HEAD_DIM] = res[:, kw + c * HEAD_DIM:kw + (c + 1) * HEAD_DIM]

        if first:
            load_kv(2)
        else:
            @pl.when(t + 2 < chips)
            def _():
                load_kv(t + 2)

            @pl.when(t + 2 >= chips)
            def _():
                load_q(t + 2 - chips)

        if first:
            pltpu.make_async_copy(dy_hbm, dy_v, in_sem.at[1]).start()
        else:
            @pl.when(t < 3)
            def _():
                load_do(t - 1)

        if first:
            pl.semaphore_wait(barrier, n - 1)
        for c in range(CORES):
            peer = ch * CORES + (core + c) % CORES

            @pl.when(peer != me)
            def _():
                peer_at(M_KV, kv_s.at[peer], kv_r.at[rows_of(me)], peer).start()
        return carry

    kv_step(0, 0, first=True)
    lax.fori_loop(1, chips, kv_step, 0)
    wait_on(dy_v, in_sem.at[1])

    def send_heads(kind, stage, dest, ch):
        for c in range(CORES):
            peer = ch * CORES + (core + c) % CORES

            @pl.when(peer != me)
            def _():
                peer_at(kind, stage.at[peer], dest.at[rows_of(me)], peer).start()

    def qdo_step(t, carry):
        ch = dest_chip(t)
        wait_on(wa.at[t % 2], a_sem.at[t % 2])
        for i in range(cw // rows):
            res = dot_nn(x_v[...], wa[t % 2, :, i * rows:(i + 1) * rows]).astype(jnp.bfloat16)
            for j in range(rows // HEAD_DIM):
                place = i * (rows // HEAD_DIM) + j
                q_s[ch * CORES + place // group, :, (place % group) * HEAD_DIM:(place % group + 1) * HEAD_DIM] = res[:, j * HEAD_DIM:(j + 1) * HEAD_DIM]

        @pl.when(t + 2 < chips)
        def _():
            load_q(t + 2)

        @pl.when(t + 2 >= chips)
        def _():
            load_dxq(t + 2 - chips)

        send_heads(M_Q, q_s, q_r, ch)
        wait_on(wb.at[t % 2], b_sem.at[t % 2])
        for i in range(cw // rows):
            res = dot_nt(dy_v[...], wb[t % 2, i * rows:(i + 1) * rows, :]).astype(jnp.bfloat16)
            for j in range(rows // HEAD_DIM):
                place = i * (rows // HEAD_DIM) + j
                do_s[ch * CORES + place // group, :, (place % group) * HEAD_DIM:(place % group + 1) * HEAD_DIM] = res[:, j * HEAD_DIM:(j + 1) * HEAD_DIM]

        @pl.when(t + 2 < chips)
        def _():
            load_do(t + 2)

        @pl.when(t + 2 >= chips)
        def _():
            load_y(t + 2 - chips)

        send_heads(M_DO, do_s, do_r, ch)
        return carry

    lax.fori_loop(0, chips, qdo_step, 0)

    kv_r[rows_of(me), :] = kv_s[me]
    q_r[rows_of(me), :] = q_s[me]
    do_r[rows_of(me), :] = do_s[me]
    dk_v[...] = jnp.zeros_like(dk_v)
    dv_v[...] = jnp.zeros_like(dv_v)

    for r in range(1, n):
        src = (me + r) % n
        recv_wait(M_KV, kv_r.at[rows_of(src)], src)

    def turn(j, carry):
        kt[:, cols_of(j, rows)] = kv_r[rows_of(j), 0:HEAD_DIM].T
        vt[:, cols_of(j, rows)] = kv_r[rows_of(j), HEAD_DIM:2 * HEAD_DIM].T
        return carry

    lax.fori_loop(0, n, turn, 0)

    kk = scale * LOG2E
    chunks = [slice(i * CHUNK, (i + 1) * CHUNK) for i in range(tokens // CHUNK)]
    k_cols, v_cols = slice(0, HEAD_DIM), slice(HEAD_DIM, 2 * HEAD_DIM)

    def source(k):
        if chips != 4:
            c_off, o_off = (chips - k // CORES) % chips, k % CORES
        else:
            near = k // 4
            c_off = near * (3 - 2 * (k % 2)) + (1 - near) * 2 * (k // 2)
            o_off = near * (k // 2 - 2) + (1 - near) * (k % 2)
        return ((chip - c_off + chips) % chips) * CORES + (core + o_off) % CORES

    def by_eights(value):
        return value.reshape(value.shape[0] // 8, 8, value.shape[1])

    def score_steps(k, probs):
        src = source(k)
        for g in range(group):
            s_ref = s_v.at[g % 2]
            st = {}

            def first(g=g, st=st):
                st["q_t"] = q_r[rows_of(src), g * HEAD_DIM:(g + 1) * HEAD_DIM].T
                st["top"] = None

            def product(sl, s_ref=s_ref, st=st):
                s_i = dot_nn(kv_r[sl, k_cols], st["q_t"])
                s_ref[sl, :] = s_i
                top = jnp.max(by_eights(s_i), axis=0)
                st["top"] = top if st["top"] is None else jnp.maximum(st["top"], top)

            def shift(st=st):
                st["mk"] = jnp.max(st["top"], axis=0, keepdims=True) * kk
                st["sum"] = None

            def add(sl, s_ref=s_ref, st=st):
                part = jnp.sum(by_eights(jnp.exp2(s_ref[sl, :] * kk - st["mk"])), axis=0)
                st["sum"] = part if st["sum"] is None else st["sum"] + part

            def close(st=st):
                st["lse"] = st["mk"] + jnp.log2(jnp.sum(st["sum"], axis=0, keepdims=True))

            def emit(sl, g=g, s_ref=s_ref, st=st):
                probs[g, sl, :] = jnp.exp2(s_ref[sl, :] * kk - st["lse"]).astype(jnp.bfloat16)

            yield 1, first
            for sl in chunks:
                yield 6, functools.partial(product, sl)
            yield 1, shift
            for sl in chunks:
                yield 6, functools.partial(add, sl)
            yield 1, close
            for sl in chunks:
                yield 6, functools.partial(emit, sl)

    def grad_steps(k, probs):
        src = source(k)
        for g in range(group):
            st = {}
            head = slice(g * HEAD_DIM, (g + 1) * HEAD_DIM)

            def outputs(g=g, head=head, st=st):
                do_t = do_r[rows_of(src), head].T
                o_t = dot_nn(vt[...], probs[g]).astype(jnp.bfloat16)
                o_s[rows_of(src), head] = o_t.T
                st["do_t"] = do_t
                st["delta"] = jnp.sum(do_t.astype(jnp.float32) * o_t.astype(jnp.float32), axis=0, keepdims=True)

            def dscore(sl, g=g, st=st):
                dp = dot_nn(kv_r[sl, v_cols], st["do_t"])
                ds_v[g, sl, :] = (probs[g, sl, :].astype(jnp.float32) * (dp - st["delta"])).astype(jnp.bfloat16)

            def dquery(g=g, head=head):
                dq_t = (dot_nn(kt[...], ds_v[g]) * scale).astype(jnp.bfloat16)
                dq_s[rows_of(src), head] = dq_t.T

            yield 12, outputs
            for sl in chunks:
                yield 4, functools.partial(dscore, sl)
            yield 10, dquery

        def accumulate(acc, left, right_ref, sl):
            total = acc[sl, :]
            part = None
            for g in range(group):
                term = dot_nn(left[g, sl, :], right_ref[rows_of(src), g * HEAD_DIM:(g + 1) * HEAD_DIM])
                part = term if part is None else part + term
            acc[sl, :] = total + part

        for sl in chunks:
            yield 12, functools.partial(accumulate, dv_v, probs, do_r, sl)
        for sl in chunks:
            yield 12, functools.partial(accumulate, dk_v, ds_v, q_r, sl)

    def run_steps(*streams):
        lists = [list(s) for s in streams]
        totals = [sum(w for w, _ in s) for s in lists]
        tagged = []
        for order, (steps, whole) in enumerate(zip(lists, totals)):
            at = 0
            for w, f in steps:
                tagged.append(((at + w / 2) / whole, order, len(tagged), f))
                at += w
        for _, _, _, f in sorted(tagged, key=lambda t: t[:3]):
            f()

    def need(kind, dest, k):
        src = source(k)

        @pl.when((k > 0) & (k < n))
        def _():
            recv_wait(kind, dest.at[rows_of(src)], src)


    def attend(k, carry):
        need(M_Q, q_r, k)
        need(M_DO, do_r, k)
        run_steps(score_steps(k, p_v.at[0])); run_steps(grad_steps(k, p_v.at[0]))
        src = source(k)

        @pl.when(k > 0)
        def _():
            peer_at(M_O, o_s.at[rows_of(src)], o_r.at[:, cols_of(me, gw)], src).start()
            peer_at(M_DQ, dq_s.at[rows_of(src)], dq_r.at[:, cols_of(me, gw)], src).start()
        return carry

    lax.fori_loop(0, n, attend, 0)

    def dk_place(owner, which):
        return cols_of((owner // CORES) * 2 * CORES + which * CORES + owner % CORES, HEAD_DIM)

    def dk_s(owner):
        return p_v.at[0, 0, rows_of(owner), 0:HEAD_DIM]

    def dv_s(owner):
        return p_v.at[0, 0, rows_of(owner), HEAD_DIM:2 * HEAD_DIM]

    def finish(j, carry):
        dst = ((chip + gray(chips - 1 - j // CORES, chips)) % chips) * CORES + (core + 1 + j % CORES) % CORES
        dk_s(dst)[...] = (dk_v[rows_of(dst), :] * scale).astype(jnp.bfloat16)
        dv_s(dst)[...] = dv_v[rows_of(dst), :].astype(jnp.bfloat16)

        @pl.when(dst != me)
        def _():
            peer_at(M_DK, dk_s(dst), dkv_r.at[:, dk_place(me, 0)], dst).start()
            peer_at(M_DV, dv_s(dst), dkv_r.at[:, dk_place(me, 1)], dst).start()
        return carry

    lax.fori_loop(0, n, finish, 0)

    o_r[:, cols_of(me, gw)] = o_s[rows_of(me), :]
    dq_r[:, cols_of(me, gw)] = dq_s[rows_of(me), :]
    dkv_r[:, dk_place(me, 0)] = dk_s(me)[...]
    dkv_r[:, dk_place(me, 1)] = dv_s(me)[...]
    pieces = d_model // rows
    y_acc[...] = jnp.zeros_like(y_acc)

    def dx_ref(c):
        return s_v.at[c // n, (c % n) * rows:(c % n + 1) * rows, :]

    for c in range(pieces):
        dx_ref(c)[...] = jnp.zeros((rows, rows), jnp.float32)

    def from_chip(t, wait):
        for c in range(CORES):
            src = home_chip(t) * CORES + (core + 1 + c) % CORES

            @pl.when(src != me)
            def _():
                wait(src)

    def wait_dkv(src):
        recv_wait(M_DK, dkv_r.at[:, dk_place(src, 0)], src)
        recv_wait(M_DV, dkv_r.at[:, dk_place(src, 1)], src)

    def back_step(t, carry):
        ch = home_chip(t)
        wait_on(wb.at[t % 2], b_sem.at[t % 2])
        from_chip(t, lambda src: recv_wait(M_O, o_r.at[:, cols_of(src, gw)], src))
        left = o_r[:, cols_of(ch, cw)]
        for c in range(pieces // PIECE):
            sl = slice(c * PIECE * rows, (c + 1) * PIECE * rows)
            y_acc[:, sl] += dot_nn(left, wb[t % 2, :, sl])

        @pl.when(t + 2 < chips)
        def _():
            load_y(t + 2)

        wait_on(wa.at[t % 2], a_sem.at[t % 2])
        from_chip(t, lambda src: recv_wait(M_DQ, dq_r.at[:, cols_of(src, gw)], src))
        left = dq_r[:, cols_of(ch, cw)]
        for c in range(pieces):
            dx_ref(c)[...] += dot_nt(left, wa[t % 2, c * rows:(c + 1) * rows, :])

        @pl.when(t + 2 < chips)
        def _():
            load_dxq(t + 2)

        @pl.when(t + 2 >= chips)
        def _():
            load_dxkv(t + 2 - chips)
        return carry

    lax.fori_loop(0, chips, back_step, 0)

    for i in range(tiles):
        y_out[:, i * cw:(i + 1) * cw] = y_acc[:, i * cw:(i + 1) * cw].astype(jnp.bfloat16)

    def dxkv_step(t, carry):
        ch = home_chip(t)
        wait_on(wa.at[t % 2, :, 0:2 * kw], a_sem.at[t % 2])
        from_chip(t, wait_dkv)
        left = dkv_r[:, cols_of(ch, 2 * kw)]
        for c in range(pieces):
            dx_ref(c)[...] += dot_nt(left, wa[t % 2, c * rows:(c + 1) * rows, 0:2 * kw])

        @pl.when(t + 2 < chips)
        def _():
            load_dxkv(t + 2)
        return carry

    lax.fori_loop(0, chips - 1, dxkv_step, 0)
    last = chips - 1
    wait_on(wa.at[last % 2, :, 0:2 * kw], a_sem.at[last % 2])
    from_chip(last, wait_dkv)
    left = dkv_r[:, cols_of(home_chip(last), 2 * kw)]
    for c in range(pieces):
        done = dx_ref(c)[...] + dot_nt(left, wa[last % 2, c * rows:(c + 1) * rows, 0:2 * kw])
        dx_out[:, c * rows:(c + 1) * rows] = done.astype(jnp.bfloat16)

    for r in range(1, n):
        peer = (me + r) % n
        peer_at(M_KV, kv_s.at[peer], kv_r.at[rows_of(me)], peer).wait_send()
        peer_at(M_Q, q_s.at[peer], q_r.at[rows_of(me)], peer).wait_send()
        peer_at(M_DO, do_s.at[peer], do_r.at[rows_of(me)], peer).wait_send()
        peer_at(M_O, o_s.at[rows_of(peer)], o_r.at[:, cols_of(me, gw)], peer).wait_send()
        peer_at(M_DQ, dq_s.at[rows_of(peer)], dq_r.at[:, cols_of(me, gw)], peer).wait_send()
        peer_at(M_DK, dk_s(peer), dkv_r.at[:, dk_place(me, 0)], peer).wait_send()
        peer_at(M_DV, dv_s(peer), dkv_r.at[:, dk_place(me, 1)], peer).wait_send()


def solution(mesh):
    n = mesh.shape["cp"]
    row_spec = P(("dp", "cp"), None)
    full_spec = P(None, None)

    def local_body(x_loc, dy_loc, w_q, w_k, w_v, w_o):
        rows, d_model = x_loc.shape
        q_heads = w_q.shape[1] // HEAD_DIM
        kv_heads = w_k.shape[1] // HEAD_DIM
        group = q_heads // kv_heads
        assert kv_heads == n and n % CORES == 0
        gw = group * HEAD_DIM
        cw = CORES * gw
        assert q_heads * HEAD_DIM == d_model and d_model % rows == 0 and d_model // rows <= 2 * n and d_model % (2 * cw) == 0
        tokens = n * rows
        bf, f32 = jnp.bfloat16, jnp.float32
        vm = pltpu.VMEM
        scratch = [
            vm((rows, d_model), bf), vm((rows, d_model), bf),
            vm((2, d_model, cw), bf), vm((2, cw, d_model), bf),
            vm((n, rows, 2 * HEAD_DIM), bf), vm((n, rows, gw), bf), vm((n, rows, gw), bf),
            vm((tokens, 2 * HEAD_DIM), bf), vm((tokens, gw), bf), vm((tokens, gw), bf),
            vm((HEAD_DIM, tokens), bf), vm((HEAD_DIM, tokens), bf),
            vm((tokens, gw), bf), vm((tokens, gw), bf),
            vm((rows, n * gw), bf), vm((rows, n * gw), bf),
            vm((tokens, HEAD_DIM), f32), vm((tokens, HEAD_DIM), f32),
            vm((rows, 2 * n * HEAD_DIM), bf),
            vm((2, tokens, rows), f32),
            vm((1, group, tokens, rows), bf), vm((group, tokens, rows), bf),
            vm((rows, d_model), f32),
            pltpu.SemaphoreType.DMA((2,)), pltpu.SemaphoreType.DMA((2,)), pltpu.SemaphoreType.DMA((2,)),
            pltpu.SemaphoreType.DMA((N_KINDS, n)), pltpu.SemaphoreType.DMA((N_KINDS, n)),
        ]
        out = pltpu.VMEM((rows, d_model), bf)
        return pl.pallas_call(
            functools.partial(body, n, rows, d_model, group),
            out_shape=(out, out),
            in_specs=[pl.BlockSpec(memory_space=pl.ANY)] * 6,
            out_specs=(pl.BlockSpec(memory_space=pltpu.VMEM), pl.BlockSpec(memory_space=pltpu.VMEM)),
            scratch_shapes=scratch,
            compiler_params=pltpu.CompilerParams(collective_id=0, has_side_effects=True,
                                                 vmem_limit_bytes=60 * 1024 * 1024),
        )(x_loc, dy_loc, w_q, w_k, w_v, w_o)

    return jax.shard_map(local_body, mesh=mesh,
                         in_specs=(row_spec, row_spec, full_spec, full_spec, full_spec, full_spec),
                         out_specs=(row_spec, row_spec), check_vma=False)
```

```python
import functools

import jax
import jax.numpy as jnp
from jax import lax
from jax.experimental import pallas as pl
from jax.experimental.pallas import tpu as pltpu
from jax.sharding import PartitionSpec as P

HEAD_DIM = 128
CORES = 2
LOG2E = 1.4426950408889634
M_KV, M_Q, M_DO, M_O, M_DQ, M_DK, M_DV = range(7)
N_KINDS = 7
PARTS = 4
PIECE = 1
CHUNK = 1024


def gray(q, n_chips):
    if n_chips != 4:
        return q
    return q + (q // 2) * (1 - 2 * (q % 2))


def dot_nn(a, b):
    return lax.dot_general(a, b, (((1,), (0,)), ((), ())), preferred_element_type=jnp.float32)


def dot_nt(a, b):
    return lax.dot_general(a, b, (((1,), (1,)), ((), ())), preferred_element_type=jnp.float32)


def body(n, rows, d_model, group,
         x_hbm, dy_hbm, wq_hbm, wk_hbm, wv_hbm, wo_hbm,
         y_out, dx_out,
         x_v, dy_v, wa, wb, kv_s, q_s, do_s, kv_r, q_r, do_r, kt, vt,
         o_s, dq_s, o_r, dq_r, dk_v, dv_v, dk_st, dv_st, dkv_r,
         s_v, p_v, ds_v, y_acc,
         in_sem, a_sem, b_sem, send_sem, recv_sem):
    chips = n // CORES
    gw = group * HEAD_DIM
    cw = CORES * gw
    kw = CORES * HEAD_DIM
    tokens = n * rows
    scale = HEAD_DIM ** -0.5
    tiles = d_model // cw
    me = lax.axis_index("cp")
    chip = me // CORES
    core = me % CORES

    def peer_at(kind, src, dst, peer):
        return pltpu.make_async_remote_copy(
            src_ref=src, dst_ref=dst, send_sem=send_sem.at[kind, peer], recv_sem=recv_sem.at[kind, me],
            device_id={"cp": peer}, device_id_type=pl.DeviceIdType.MESH)

    def recv_wait(kind, dst, peer):
        pltpu.make_async_remote_copy(
            src_ref=dst, dst_ref=dst, send_sem=send_sem.at[kind, peer], recv_sem=recv_sem.at[kind, peer],
            device_id={"cp": peer}, device_id_type=pl.DeviceIdType.MESH).wait_recv()

    def rows_of(i):
        return pl.ds(pl.multiple_of(i * rows, rows), rows)

    def cols_of(i, w):
        return pl.ds(pl.multiple_of(i * w, w), w)

    def dest_chip(t):
        return (chip + gray(chips - 1 - t, chips)) % chips

    def start_parts(src, dst, sem, n_rows):
        step = n_rows // PARTS
        for i in range(PARTS):
            pltpu.make_async_copy(src.at[i * step:(i + 1) * step], dst.at[i * step:(i + 1) * step], sem).start()

    def load_kv(t):
        ch = dest_chip(t)
        a_t = wa.at[t % 2]
        start_parts(wk_hbm.at[:, cols_of(ch, kw)], a_t.at[:, 0:kw], a_sem.at[t % 2], d_model)
        start_parts(wv_hbm.at[:, cols_of(ch, kw)], a_t.at[:, kw:2 * kw], a_sem.at[t % 2], d_model)

    def load_q(t):
        start_parts(wq_hbm.at[:, cols_of(dest_chip(t), cw)], wa.at[t % 2], a_sem.at[t % 2], d_model)

    def load_do(t):
        start_parts(wo_hbm.at[cols_of(dest_chip(t), cw)], wb.at[t % 2], b_sem.at[t % 2], cw)

    def home_chip(t):
        return (chip + gray((chips - t) % chips, chips)) % chips

    def load_y(t):
        start_parts(wo_hbm.at[cols_of(home_chip(t), cw)], wb.at[t % 2], b_sem.at[t % 2], cw)

    def load_dxq(t):
        start_parts(wq_hbm.at[:, cols_of(home_chip(t), cw)], wa.at[t % 2], a_sem.at[t % 2], d_model)

    def load_dxkv(t):
        a_t = wa.at[t % 2]
        start_parts(wk_hbm.at[:, cols_of(home_chip(t), kw)], a_t.at[:, 0:kw], a_sem.at[t % 2], d_model)
        start_parts(wv_hbm.at[:, cols_of(home_chip(t), kw)], a_t.at[:, kw:2 * kw], a_sem.at[t % 2], d_model)

    def wait_on(ref, sem):
        pltpu.make_async_copy(ref, ref, sem).wait()

    pltpu.make_async_copy(x_hbm, x_v, in_sem.at[0]).start()
    load_kv(0)

    barrier = pltpu.get_barrier_semaphore()
    for r in range(1, n):
        pl.semaphore_signal(barrier, inc=1, device_id={"cp": (me + r) % n}, device_id_type=pl.DeviceIdType.MESH)
    load_kv(1)

    wait_on(x_v, in_sem.at[0])

    def kv_step(t, carry, first=False):
        ch = dest_chip(t)
        wait_on(wa.at[t % 2, :, 0:2 * kw], a_sem.at[t % 2])
        res = dot_nn(x_v[...], wa[t % 2, :, 0:2 * kw]).astype(jnp.bfloat16)
        for c in range(CORES):
            kv_s[ch * CORES + c, :, 0:HEAD_DIM] = res[:, c * HEAD_DIM:(c + 1) * HEAD_DIM]
            kv_s[ch * CORES + c, :, HEAD_DIM:2 * HEAD_DIM] = res[:, kw + c * HEAD_DIM:kw + (c + 1) * HEAD_DIM]

        if first:
            load_kv(2)
        else:
            @pl.when(t + 2 < chips)
            def _():
                load_kv(t + 2)

            @pl.when(t + 2 >= chips)
            def _():
                load_q(t + 2 - chips)

        if first:
            pltpu.make_async_copy(dy_hbm, dy_v, in_sem.at[1]).start()
        else:
            @pl.when(t < 3)
            def _():
                load_do(t - 1)

        if first:
            pl.semaphore_wait(barrier, n - 1)
        for c in range(CORES):
            peer = ch * CORES + (core + c) % CORES

            @pl.when(peer != me)
            def _():
                peer_at(M_KV, kv_s.at[peer], kv_r.at[rows_of(me)], peer).start()
        return carry

    kv_step(0, 0, first=True)
    lax.fori_loop(1, chips, kv_step, 0)
    wait_on(dy_v, in_sem.at[1])

    def send_heads(kind, stage, dest, ch):
        for c in range(CORES):
            peer = ch * CORES + (core + c) % CORES

            @pl.when(peer != me)
            def _():
                peer_at(kind, stage.at[peer], dest.at[rows_of(me)], peer).start()

    def qdo_step(t, carry):
        ch = dest_chip(t)
        wait_on(wa.at[t % 2], a_sem.at[t % 2])
        for i in range(cw // rows):
            res = dot_nn(x_v[...], wa[t % 2, :, i * rows:(i + 1) * rows]).astype(jnp.bfloat16)
            for j in range(rows // HEAD_DIM):
                place = i * (rows // HEAD_DIM) + j
                q_s[ch * CORES + place // group, :, (place % group) * HEAD_DIM:(place % group + 1) * HEAD_DIM] = res[:, j * HEAD_DIM:(j + 1) * HEAD_DIM]

        @pl.when(t + 2 < chips)
        def _():
            load_q(t + 2)

        @pl.when(t + 2 >= chips)
        def _():
            load_dxq(t + 2 - chips)

        send_heads(M_Q, q_s, q_r, ch)
        wait_on(wb.at[t % 2], b_sem.at[t % 2])
        for i in range(cw // rows):
            res = dot_nt(dy_v[...], wb[t % 2, i * rows:(i + 1) * rows, :]).astype(jnp.bfloat16)
            for j in range(rows // HEAD_DIM):
                place = i * (rows // HEAD_DIM) + j
                do_s[ch * CORES + place // group, :, (place % group) * HEAD_DIM:(place % group + 1) * HEAD_DIM] = res[:, j * HEAD_DIM:(j + 1) * HEAD_DIM]

        @pl.when(t + 2 < chips)
        def _():
            load_do(t + 2)

        @pl.when(t + 2 >= chips)
        def _():
            load_y(t + 2 - chips)

        send_heads(M_DO, do_s, do_r, ch)
        return carry

    lax.fori_loop(0, chips, qdo_step, 0)

    kv_r[rows_of(me), :] = kv_s[me]
    q_r[rows_of(me), :] = q_s[me]
    do_r[rows_of(me), :] = do_s[me]
    dk_v[...] = jnp.zeros_like(dk_v)
    dv_v[...] = jnp.zeros_like(dv_v)

    for r in range(1, n):
        src = (me + r) % n
        recv_wait(M_KV, kv_r.at[rows_of(src)], src)

    def turn(j, carry):
        kt[:, cols_of(j, rows)] = kv_r[rows_of(j), 0:HEAD_DIM].T
        vt[:, cols_of(j, rows)] = kv_r[rows_of(j), HEAD_DIM:2 * HEAD_DIM].T
        return carry

    lax.fori_loop(0, n, turn, 0)

    kk = scale * LOG2E
    chunks = [slice(i * CHUNK, (i + 1) * CHUNK) for i in range(tokens // CHUNK)]
    k_cols, v_cols = slice(0, HEAD_DIM), slice(HEAD_DIM, 2 * HEAD_DIM)

    def source(k):
        if chips != 4:
            c_off, o_off = (chips - k // CORES) % chips, k % CORES
        else:
            near = k // 4
            c_off = near * (3 - 2 * (k % 2)) + (1 - near) * 2 * (k // 2)
            o_off = near * (k // 2 - 2) + (1 - near) * (k % 2)
        return ((chip - c_off + chips) % chips) * CORES + (core + o_off) % CORES

    def by_eights(value):
        return value.reshape(value.shape[0] // 8, 8, value.shape[1])

    def score_steps(k, probs):
        src = source(k)
        for g in range(group):
            s_ref = s_v.at[g % 2]
            st = {}

            def first(g=g, st=st):
                st["q_t"] = q_r[rows_of(src), g * HEAD_DIM:(g + 1) * HEAD_DIM].T
                st["top"] = None

            def product(sl, s_ref=s_ref, st=st):
                s_i = dot_nn(kv_r[sl, k_cols], st["q_t"])
                s_ref[sl, :] = s_i
                top = jnp.max(by_eights(s_i), axis=0)
                st["top"] = top if st["top"] is None else jnp.maximum(st["top"], top)

            def shift(st=st):
                st["mk"] = jnp.max(st["top"], axis=0, keepdims=True) * kk
                st["sum"] = None

            def add(sl, s_ref=s_ref, st=st):
                part = jnp.sum(by_eights(jnp.exp2(s_ref[sl, :] * kk - st["mk"])), axis=0)
                st["sum"] = part if st["sum"] is None else st["sum"] + part

            def close(st=st):
                st["lse"] = st["mk"] + jnp.log2(jnp.sum(st["sum"], axis=0, keepdims=True))

            def emit(sl, g=g, s_ref=s_ref, st=st):
                probs[g, sl, :] = jnp.exp2(s_ref[sl, :] * kk - st["lse"]).astype(jnp.bfloat16)

            yield 1, first
            for sl in chunks:
                yield 6, functools.partial(product, sl)
            yield 1, shift
            for sl in chunks:
                yield 6, functools.partial(add, sl)
            yield 1, close
            for sl in chunks:
                yield 6, functools.partial(emit, sl)

    def grad_steps(k, probs):
        src = source(k)
        for g in range(group):
            st = {}
            head = slice(g * HEAD_DIM, (g + 1) * HEAD_DIM)

            def outputs(g=g, head=head, st=st):
                do_t = do_r[rows_of(src), head].T
                o_t = dot_nn(vt[...], probs[g]).astype(jnp.bfloat16)
                o_s[rows_of(src), head] = o_t.T
                st["do_t"] = do_t
                st["delta"] = jnp.sum(do_t.astype(jnp.float32) * o_t.astype(jnp.float32), axis=0, keepdims=True)

            def dscore(sl, g=g, st=st):
                dp = dot_nn(kv_r[sl, v_cols], st["do_t"])
                ds_v[g, sl, :] = (probs[g, sl, :].astype(jnp.float32) * (dp - st["delta"])).astype(jnp.bfloat16)

            def dquery(g=g, head=head):
                dq_t = (dot_nn(kt[...], ds_v[g]) * scale).astype(jnp.bfloat16)
                dq_s[rows_of(src), head] = dq_t.T

            yield 12, outputs
            for sl in chunks:
                yield 4, functools.partial(dscore, sl)
            yield 10, dquery

        def accumulate(acc, left, right_ref, sl):
            total = acc[sl, :]
            part = None
            for g in range(group):
                term = dot_nn(left[g, sl, :], right_ref[rows_of(src), g * HEAD_DIM:(g + 1) * HEAD_DIM])
                part = term if part is None else part + term
            acc[sl, :] = total + part

        for sl in chunks:
            yield 12, functools.partial(accumulate, dv_v, probs, do_r, sl)
        for sl in chunks:
            yield 12, functools.partial(accumulate, dk_v, ds_v, q_r, sl)

    def run_steps(*streams):
        lists = [list(s) for s in streams]
        totals = [sum(w for w, _ in s) for s in lists]
        tagged = []
        for order, (steps, whole) in enumerate(zip(lists, totals)):
            at = 0
            for w, f in steps:
                tagged.append(((at + w / 2) / whole, order, len(tagged), f))
                at += w
        for _, _, _, f in sorted(tagged, key=lambda t: t[:3]):
            f()

    def need(kind, dest, k):
        src = source(k)

        @pl.when((k > 0) & (k < n))
        def _():
            recv_wait(kind, dest.at[rows_of(src)], src)


    def attend(k, carry):
        need(M_Q, q_r, k)
        need(M_DO, do_r, k)
        run_steps(score_steps(k, p_v.at[0])); run_steps(grad_steps(k, p_v.at[0]))
        src = source(k)

        @pl.when(k > 0)
        def _():
            peer_at(M_O, o_s.at[rows_of(src)], o_r.at[:, cols_of(me, gw)], src).start()
            peer_at(M_DQ, dq_s.at[rows_of(src)], dq_r.at[:, cols_of(me, gw)], src).start()
        return carry

    lax.fori_loop(0, n, attend, 0)

    def dk_place(owner, which):
        return cols_of((owner // CORES) * 2 * CORES + which * CORES + owner % CORES, HEAD_DIM)

    def dk_s(owner):
        return dk_st.at[owner]

    def dv_s(owner):
        return dv_st.at[owner]

    def finish(j, carry):
        dst = ((chip + gray(chips - 1 - j // CORES, chips)) % chips) * CORES + (core + 1 + j % CORES) % CORES
        dk_s(dst)[...] = (dk_v[rows_of(dst), :] * scale).astype(jnp.bfloat16)
        dv_s(dst)[...] = dv_v[rows_of(dst), :].astype(jnp.bfloat16)

        @pl.when(dst != me)
        def _():
            peer_at(M_DK, dk_s(dst), dkv_r.at[:, dk_place(me, 0)], dst).start()
            peer_at(M_DV, dv_s(dst), dkv_r.at[:, dk_place(me, 1)], dst).start()
        return carry

    lax.fori_loop(0, n, finish, 0)

    o_r[:, cols_of(me, gw)] = o_s[rows_of(me), :]
    dq_r[:, cols_of(me, gw)] = dq_s[rows_of(me), :]
    dkv_r[:, dk_place(me, 0)] = dk_s(me)[...]
    dkv_r[:, dk_place(me, 1)] = dv_s(me)[...]
    pieces = d_model // rows
    y_acc[...] = jnp.zeros_like(y_acc)

    def dx_ref(c):
        return s_v.at[c // n, (c % n) * rows:(c % n + 1) * rows, :]

    for c in range(pieces):
        dx_ref(c)[...] = jnp.zeros((rows, rows), jnp.float32)

    def from_chip(t, wait):
        for c in range(CORES):
            src = home_chip(t) * CORES + (core + 1 + c) % CORES

            @pl.when(src != me)
            def _():
                wait(src)

    def wait_dkv(src):
        recv_wait(M_DK, dkv_r.at[:, dk_place(src, 0)], src)
        recv_wait(M_DV, dkv_r.at[:, dk_place(src, 1)], src)

    def back_step(t, carry):
        ch = home_chip(t)
        wait_on(wb.at[t % 2], b_sem.at[t % 2])
        from_chip(t, lambda src: recv_wait(M_O, o_r.at[:, cols_of(src, gw)], src))
        left = o_r[:, cols_of(ch, cw)]
        for c in range(pieces // PIECE):
            sl = slice(c * PIECE * rows, (c + 1) * PIECE * rows)
            y_acc[:, sl] += dot_nn(left, wb[t % 2, :, sl])

        @pl.when(t + 2 < chips)
        def _():
            load_y(t + 2)

        wait_on(wa.at[t % 2], a_sem.at[t % 2])
        from_chip(t, lambda src: recv_wait(M_DQ, dq_r.at[:, cols_of(src, gw)], src))
        left = dq_r[:, cols_of(ch, cw)]
        for c in range(pieces):
            dx_ref(c)[...] += dot_nt(left, wa[t % 2, c * rows:(c + 1) * rows, :])

        @pl.when(t + 2 < chips)
        def _():
            load_dxq(t + 2)

        @pl.when(t + 2 >= chips)
        def _():
            load_dxkv(t + 2 - chips)
        return carry

    lax.fori_loop(0, chips, back_step, 0)

    for i in range(tiles):
        y_out[:, i * cw:(i + 1) * cw] = y_acc[:, i * cw:(i + 1) * cw].astype(jnp.bfloat16)

    def dxkv_step(t, carry):
        ch = home_chip(t)
        wait_on(wa.at[t % 2, :, 0:2 * kw], a_sem.at[t % 2])
        from_chip(t, wait_dkv)
        left = dkv_r[:, cols_of(ch, 2 * kw)]
        for c in range(pieces):
            dx_ref(c)[...] += dot_nt(left, wa[t % 2, c * rows:(c + 1) * rows, 0:2 * kw])

        @pl.when(t + 2 < chips)
        def _():
            load_dxkv(t + 2)
        return carry

    lax.fori_loop(0, chips - 1, dxkv_step, 0)
    last = chips - 1
    wait_on(wa.at[last % 2, :, 0:2 * kw], a_sem.at[last % 2])
    from_chip(last, wait_dkv)
    left = dkv_r[:, cols_of(home_chip(last), 2 * kw)]
    for c in range(pieces):
        done = dx_ref(c)[...] + dot_nt(left, wa[last % 2, c * rows:(c + 1) * rows, 0:2 * kw])
        dx_out[:, c * rows:(c + 1) * rows] = done.astype(jnp.bfloat16)

    for r in range(1, n):
        peer = (me + r) % n
        peer_at(M_KV, kv_s.at[peer], kv_r.at[rows_of(me)], peer).wait_send()
        peer_at(M_Q, q_s.at[peer], q_r.at[rows_of(me)], peer).wait_send()
        peer_at(M_DO, do_s.at[peer], do_r.at[rows_of(me)], peer).wait_send()
        peer_at(M_O, o_s.at[rows_of(peer)], o_r.at[:, cols_of(me, gw)], peer).wait_send()
        peer_at(M_DQ, dq_s.at[rows_of(peer)], dq_r.at[:, cols_of(me, gw)], peer).wait_send()
        peer_at(M_DK, dk_s(peer), dkv_r.at[:, dk_place(me, 0)], peer).wait_send()
        peer_at(M_DV, dv_s(peer), dkv_r.at[:, dk_place(me, 1)], peer).wait_send()


def solution(mesh):
    n = mesh.shape["cp"]
    row_spec = P(("dp", "cp"), None)
    full_spec = P(None, None)

    def local_body(x_loc, dy_loc, w_q, w_k, w_v, w_o):
        rows, d_model = x_loc.shape
        q_heads = w_q.shape[1] // HEAD_DIM
        kv_heads = w_k.shape[1] // HEAD_DIM
        group = q_heads // kv_heads
        assert kv_heads == n and n % CORES == 0
        gw = group * HEAD_DIM
        cw = CORES * gw
        assert q_heads * HEAD_DIM == d_model and d_model % rows == 0 and d_model // rows <= 2 * n and d_model % (2 * cw) == 0
        tokens = n * rows
        bf, f32 = jnp.bfloat16, jnp.float32
        vm = pltpu.VMEM
        scratch = [
            vm((rows, d_model), bf), vm((rows, d_model), bf),
            vm((2, d_model, cw), bf), vm((2, cw, d_model), bf),
            vm((n, rows, 2 * HEAD_DIM), bf), vm((n, rows, gw), bf), vm((n, rows, gw), bf),
            vm((tokens, 2 * HEAD_DIM), bf), vm((tokens, gw), bf), vm((tokens, gw), bf),
            vm((HEAD_DIM, tokens), bf), vm((HEAD_DIM, tokens), bf),
            vm((tokens, gw), bf), vm((tokens, gw), bf),
            vm((rows, n * gw), bf), vm((rows, n * gw), bf),
            vm((tokens, HEAD_DIM), f32), vm((tokens, HEAD_DIM), f32),
            vm((n, rows, HEAD_DIM), bf), vm((n, rows, HEAD_DIM), bf),
            vm((rows, 2 * n * HEAD_DIM), bf),
            vm((2, tokens, rows), f32),
            vm((1, group, tokens, rows), bf), vm((group, tokens, rows), bf),
            vm((rows, d_model), f32),
            pltpu.SemaphoreType.DMA((2,)), pltpu.SemaphoreType.DMA((2,)), pltpu.SemaphoreType.DMA((2,)),
            pltpu.SemaphoreType.DMA((N_KINDS, n)), pltpu.SemaphoreType.DMA((N_KINDS, n)),
        ]
        out = pltpu.VMEM((rows, d_model), bf)
        return pl.pallas_call(
            functools.partial(body, n, rows, d_model, group),
            out_shape=(out, out),
            in_specs=[pl.BlockSpec(memory_space=pl.ANY)] * 6,
            out_specs=(pl.BlockSpec(memory_space=pltpu.VMEM), pl.BlockSpec(memory_space=pltpu.VMEM)),
            scratch_shapes=scratch,
            compiler_params=pltpu.CompilerParams(collective_id=0, has_side_effects=True,
                                                 vmem_limit_bytes=60 * 1024 * 1024),
        )(x_loc, dy_loc, w_q, w_k, w_v, w_o)

    return jax.shard_map(local_body, mesh=mesh,
                         in_specs=(row_spec, row_spec, full_spec, full_spec, full_spec, full_spec),
                         out_specs=(row_spec, row_spec), check_vma=False)
```
